128 devices in a mesh: sta: 16 (over x, z_lo, core), win: 8 (over y, z_hi).
Axes of the slice: x: 4, y: 4, z: 4 (z_hi: 2, z_lo: 2; z = z_hi * 2 + z_lo), core: 2. Of those that a mesh axis runs over, the one named last changes fastest.
Arguments:
- green: bfloat16 [16, 3, 2, 512, 2048], P('sta', None, None, None, 'win'), may hold values from -0.02734375 to 0.02734375
- records: float32 [16, 3, 2, 2048], P('sta', None, None, 'win'), may hold values from -6 to 6
- onsets: int32 [512, 32], P('sta', 'win'), may hold values from 0 to 4095
- mask: int32 [16, 3], P('sta'), may hold values 0 or 1
Outputs:
- slip: float32 [512, 32], P('sta', 'win')
- direction: float32 [512, 32], P('sta', 'win')
- misfit: float32 [16, 3, 2, 2048], P('sta', None, None, 'win')
The draws below stay inside these ranges and needn't reach their ends.
All inputs are finite; a program needn't handle non-finite values. No bound on the sum of `mask` on one device may be relied on, other than what follows from the above.
Results may differ from the reference program's by a relative error of at most 0.007.
Values may be sent and summed in bfloat16 or wider, within the bound.
No kernel may reach another device: no remote copies, remote signals or barrier semaphores. Data moves between devices by JAX's collectives and lax.ppermute only.
A program may use at most 64 MiB of HBM per device.

```python
import math
import jax
import jax.numpy as jnp
from jax import lax

COMP = 3
WINDOWS = 32
FREQS = 2048
SAMPLES = 4096
ITERS = 2
PATCHES = 512
STATIONS = 16


def with_ends(drawn, key, low, top_value):
    place = [jax.random.randint(jax.random.fold_in(key, axis), (), 0, length) for axis, length in enumerate(drawn.shape)]
    widest = drawn.shape.index(max(drawn.shape))
    beside = place[:widest] + [(place[widest] + 1) % drawn.shape[widest]] + place[widest + 1:]
    return drawn.at[tuple(place)].set(low).at[tuple(beside)].set(top_value)


def spiked(entries, key, source, target, blocks, factor):
    owner, partner = [(jnp.arange(entries.shape[position]) // (entries.shape[position] // blocks)).reshape([-1 if axis == position else 1 for axis in range(entries.ndim)]) for position in (source, target)]
    chosen = jax.random.permutation(key, blocks)[partner]
    strong = (owner == chosen) | (owner == (partner + blocks // 2) % blocks)
    return jnp.where(strong, factor * entries, entries)


def shard_levels(key, dims, split, low, high):
    gain, own = 1.0, jax.random.fold_in(key, 6)
    for position, blocks in split:
        heights = jnp.exp(jax.random.uniform(jax.random.fold_in(own, position), (blocks,), jnp.float32, low / len(split), high / len(split)))
        gain = gain * jnp.repeat(heights, dims[position] // blocks).reshape([-1 if axis == position else 1 for axis in range(len(dims))])
    return gain


def normal_values(rng, dims, deviation, limit, cuts=(), kind=jnp.bfloat16):
    result = deviation * jax.random.normal(rng, dims, jnp.float32)
    if cuts:
        result = result * shard_levels(rng, dims, cuts, -0.22, 0.18)
    return jnp.clip(result, -limit, limit).astype(kind)


def noise_with(key, shape, scale, most, shards, heavy, held_as=jnp.bfloat16):
    entries = scale * jax.random.normal(key, shape, jnp.float32)
    if shards:
        entries = entries * shard_levels(key, shape, shards, -0.22, 0.18)
    return jnp.clip(spiked(entries, jax.random.fold_in(key, 3), *heavy), -most, most).astype(held_as)


def setup_inputs(seed: int = 0) -> dict:
    key_of = jax.random.split(jax.random.key(seed), 5)
    green = noise_with(key_of[0], (STATIONS, COMP, 2, PATCHES, FREQS), (COMP * STATIONS * FREQS) ** -0.5, 0.02734375, ((0, 16), (4, 8)), (0, 3, 16, 2.0))
    records = normal_values(key_of[1], (STATIONS, COMP, 2, FREQS), 1.0, 6.0, ((0, 16), (3, 8)), jnp.float32)
    onsets = with_ends(jax.random.randint(key_of[2], (PATCHES, WINDOWS), 0, SAMPLES), jax.random.fold_in(key_of[2], 1), 0, SAMPLES - 1).astype(jnp.int32)
    mask = with_ends((jax.random.randint(key_of[3], (STATIONS, COMP), 0, 6) < 5).astype(jnp.int32), jax.random.fold_in(key_of[3], 1), 0, 1)
    return dict(green=green, records=records, onsets=onsets, mask=mask)


TWO_PI = 2.0 * math.pi

def phase_tables(onset_block, frequency):
    turns = onset_block[:, :, None] * frequency[None, None, :] % SAMPLES
    angle = turns.astype(jnp.float32) * (TWO_PI / SAMPLES)
    return (jnp.cos(angle), jnp.sin(angle))

def spectra_from(values, cosine, sine):
    real_part = lax.optimization_barrier(jnp.sum(values[:, :, None] * cosine, axis=1))
    imag_part = -lax.optimization_barrier(jnp.sum(values[:, :, None] * sine, axis=1))
    return jnp.stack([real_part, imag_part], axis=1).astype(jnp.bfloat16)

def project_with(combined, cosine, sine):
    return lax.optimization_barrier(jnp.sum(cosine * combined[:, 0, None, :] - sine * combined[:, 1, None, :], axis=2))

def spectra(model, onsets):
    frequency = jnp.arange(FREQS, dtype=jnp.int32)
    block = math.gcd(PATCHES, 256)

    def one_block(pair):
        values, onset_block = pair
        cosine, sine = phase_tables(onset_block, frequency)
        return spectra_from(values, cosine, sine)
    blocks = lax.map(one_block, (model.reshape(-1, block, WINDOWS), onsets.reshape(-1, block, WINDOWS)))
    return blocks.reshape(PATCHES, 2, FREQS)

def project(combined, onsets):
    frequency = jnp.arange(FREQS, dtype=jnp.int32)
    block = math.gcd(PATCHES, 256)

    def one_block(pair):
        parts, onset_block = pair
        cosine, sine = phase_tables(onset_block, frequency)
        return project_with(parts, cosine, sine)
    blocks = lax.map(one_block, (combined.reshape(-1, block, 2, FREQS), onsets.reshape(-1, block, WINDOWS)))
    return blocks.reshape(PATCHES, WINDOWS)

def forward(green, spectrum, weight):
    spec_re = spectrum[:, 0, :].astype(jnp.float32)
    spec_im = spectrum[:, 1, :].astype(jnp.float32)

    def one_station(station):
        green_re = station[:, 0].astype(jnp.float32)
        green_im = station[:, 1].astype(jnp.float32)
        real_part = lax.optimization_barrier(jnp.sum(green_re * spec_re - green_im * spec_im, axis=1))
        imag_part = lax.optimization_barrier(jnp.sum(green_re * spec_im + green_im * spec_re, axis=1))
        return jnp.stack([real_part, imag_part], axis=1)
    return lax.map(one_station, green) * weight

def adjoint(green, vector, weight, onsets):
    rounded = (vector * weight).astype(jnp.bfloat16)

    def add_station(total, item):
        station, trace = item
        green_re = station[:, 0].astype(jnp.float32)
        green_im = station[:, 1].astype(jnp.float32)
        trace_re = trace[:, 0].astype(jnp.float32)[:, None, :]
        trace_im = trace[:, 1].astype(jnp.float32)[:, None, :]
        part_re = lax.optimization_barrier(jnp.sum(green_re * trace_re + green_im * trace_im, axis=0))
        part_im = lax.optimization_barrier(jnp.sum(green_re * trace_im - green_im * trace_re, axis=0))
        return (total + jnp.stack([part_re, part_im], axis=1), None)
    start_total = jnp.zeros((PATCHES, 2, FREQS), jnp.float32)
    combined, unused = lax.scan(add_station, start_total, (green, rounded))
    return project(combined, onsets)

def reference(green, records, onsets, mask):
    weight = mask.astype(jnp.float32)[:, :, None, None]
    left = records * weight
    beta_norm = jnp.sqrt(jnp.sum(left * left))
    left = left / beta_norm
    right = adjoint(green, left, weight, onsets)
    alpha_norm = jnp.sqrt(jnp.sum(right * right))
    right = right / alpha_norm
    search = right
    estimate = jnp.zeros((PATCHES, WINDOWS), jnp.float32)
    phi_bar = beta_norm
    rho_bar = alpha_norm
    for sweep in range(ITERS):
        left = forward(green, spectra(right, onsets), weight) - alpha_norm * left
        beta_norm = jnp.sqrt(jnp.sum(left * left))
        left = left / beta_norm
        right = adjoint(green, left, weight, onsets) - beta_norm * right
        alpha_norm = jnp.sqrt(jnp.sum(right * right))
        right = right / alpha_norm
        rho_value = jnp.sqrt(rho_bar * rho_bar + beta_norm * beta_norm)
        cosine_rot = rho_bar / rho_value
        sine_rot = beta_norm / rho_value
        theta_rot = sine_rot * alpha_norm
        rho_bar = -cosine_rot * alpha_norm
        phi_step = cosine_rot * phi_bar
        phi_bar = sine_rot * phi_bar
        estimate = estimate + phi_step / rho_value * search
        search = right - theta_rot / rho_value * search
    return (estimate, search * math.sqrt(PATCHES * WINDOWS), phi_bar * left)
```

```python
import functools
import math

import jax
import jax.numpy as jnp
from jax import lax
from jax.experimental import pallas as pl
from jax.experimental.pallas import tpu as pltpu
from jax.sharding import Mesh
from jax.sharding import PartitionSpec as P

X, ZL, C, Y, ZH = "x", "zl", "core", "y", "zh"
STA = (X, ZL, C)
WIN = (Y, ZH)
SAMPLES = 4096
LANES = 128
COMP = 3
PARTS = 2 * COMP
PATCHES = 64
WINDOWS = 32
GREEN_ROWS = PARTS * PATCHES
ROWS = GREEN_ROWS + 24
PACKED = 16
IMAGE = 24
SQUARES = 6
f32, bf16 = jnp.float32, jnp.bfloat16
VMEM = pl.BlockSpec(memory_space=pltpu.VMEM)
SMEM = pl.BlockSpec(memory_space=pltpu.SMEM)
PARAMS = pltpu.CompilerParams(vmem_limit_bytes=16 << 20)


def call(body, outs, *args, flops=2_000_000):
    return pl.pallas_call(
        body,
        in_specs=[SMEM if a.dtype == jnp.int32 and a.ndim == 1 else VMEM for a in args],
        out_specs=[VMEM] * len(outs),
        out_shape=[jax.ShapeDtypeStruct(s, d) for s, d in outs],
        compiler_params=PARAMS,
        cost_estimate=pl.CostEstimate(flops=flops, bytes_accessed=4_000_000, transcendentals=0),
    )(*args)


def pack_body(mask_ref, green_ref, rec_ref, out_ref, rows):
    rows[...] = jnp.zeros_like(rows)
    for comp in range(COMP):
        used = mask_ref[0, comp] != 0
        rows[2 * comp : 2 * comp + 2, :] = jnp.where(used, rec_ref[0, comp], 0.0)
        for part in range(2):
            k = 2 * comp + part
            for zl in range(2):
                for c in range(2):
                    at = zl * 64 + c * 32
                    block = green_ref[0, comp, part, at : at + 32, :]
                    block = jnp.where(used, block, jnp.zeros_like(block))
                    to = k * PATCHES + zl * 32
                    for half in range(2):
                        out_ref[0, half, c, to : to + 32, :] = block[:, half * LANES : (half + 1) * LANES]
    for half in range(2):
        rest = rows[:, half * LANES : (half + 1) * LANES]
        for term in range(3):
            piece = rest.astype(bf16)
            rest = rest - piece.astype(f32)
            at = GREEN_ROWS + 8 * term
            for c in range(2):
                out_ref[0, half, c, at : at + 8, :] = piece


def pack(mask, green, records):
    return pl.pallas_call(
        pack_body,
        grid=(4,),
        in_specs=[
            SMEM,
            pl.BlockSpec((1, COMP, 2, 128, 256), lambda i: (0, 0, 0, i, 0)),
            pl.BlockSpec((1, COMP, 2, 256), lambda i: (0, 0, 0, 0)),
        ],
        out_specs=pl.BlockSpec((1, 2, 2, ROWS, LANES), lambda i: (i, 0, 0, 0, 0)),
        out_shape=jax.ShapeDtypeStruct((4, 2, 2, ROWS, LANES), bf16),
        scratch_shapes=[pltpu.VMEM((8, 256), f32)],
        compiler_params=PARAMS,
    )(mask, green, records)


def table_body(idx_ref, onset_ref, cos_ref, sin_ref):
    first = idx_ref[3] * 256 + idx_ref[1] * LANES
    freq = lax.broadcasted_iota(jnp.int32, (PATCHES, LANES), 1) + first
    for w in range(WINDOWS):
        onset = jnp.broadcast_to(onset_ref[:, w : w + 1], (PATCHES, LANES))
        turns = onset * freq + SAMPLES // 8
        quarter = lax.shift_right_logical(turns, 10) & 3
        angle = ((turns & (SAMPLES // 4 - 1)) - SAMPLES // 8).astype(f32) * (2.0 * math.pi / SAMPLES)
        y = angle * angle
        s = angle * (1.0 + y * (-1 / 6 + y * (1 / 120 + y * (-1 / 5040 + y * (1 / 362880)))))
        c = 1.0 + y * (-0.5 + y * (1 / 24 + y * (-1 / 720 + y * (1 / 40320 + y * (-1 / 3628800)))))
        odd = (quarter & 1) == 1
        cosine = jnp.where(odd, s, c)
        sine = jnp.where(odd, c, s)
        cos_ref[w] = jnp.where((quarter == 1) | (quarter == 2), -cosine, cosine)
        sin_ref[w] = jnp.where(quarter >= 2, -sine, sine)


def model_to_data(model, ss, c, own_ref, oth_ref, cos_ref, sin_ref, data_ref, spec):
    for q in range(4):
        re = jnp.zeros((PACKED, LANES), f32)
        im = jnp.zeros((PACKED, LANES), f32)
        for w in range(WINDOWS):
            at = q * WINDOWS + w
            v = jnp.broadcast_to(model[:, at : at + 1], (PACKED, LANES))
            re = re + v * cos_ref[w, q * PACKED : (q + 1) * PACKED, :]
            im = im - v * sin_ref[w, q * PACKED : (q + 1) * PACKED, :]
        spec[0, q * PACKED : (q + 1) * PACKED, :] = re
        spec[1, q * PACKED : (q + 1) * PACKED, :] = im
    re, im = spec[0], spec[1]
    zero = jnp.zeros((2, LANES), f32)
    for ref, core in ((own_ref, c), (oth_ref, 1 - c)):

        def station(s, carry, ref=ref, core=core):
            for comp in range(COMP):
                at = 2 * comp * PATCHES
                g_re = ref[s, at : at + PATCHES, :].astype(f32)
                g_im = ref[s, at + PATCHES : at + 2 * PATCHES, :].astype(f32)
                data_ref[core * 8 + s, 2 * comp : 2 * comp + 1, :] = jnp.sum(g_re * re - g_im * im, axis=0, keepdims=True)
                data_ref[core * 8 + s, 2 * comp + 1 : 2 * comp + 2, :] = jnp.sum(g_re * im + g_im * re, axis=0, keepdims=True)
            data_ref[core * 8 + s, SQUARES:, :] = zero
            return carry

        lax.fori_loop(0, 8, station, 0)
    data_ref[0, SQUARES : SQUARES + 1, :] = ss


def data_to_model(c, u_ref, own_ref, oth_ref, cos_ref, sin_ref, buf_ref):
    total = (jnp.zeros((PATCHES, LANES), f32), jnp.zeros((PATCHES, LANES), f32))
    for ref, core in ((own_ref, c), (oth_ref, 1 - c)):

        def station(s, carry, ref=ref, core=core):
            q_re, q_im = carry
            for comp in range(COMP):
                at = 2 * comp * PATCHES
                g_re = ref[s, at : at + PATCHES, :].astype(f32)
                g_im = ref[s, at + PATCHES : at + 2 * PATCHES, :].astype(f32)
                u_re = u_ref[core * 8 + s, 2 * comp : 2 * comp + 1, :]
                u_im = u_ref[core * 8 + s, 2 * comp + 1 : 2 * comp + 2, :]
                q_re = q_re + (g_re * u_re + g_im * u_im)
                q_im = q_im + (g_re * u_im - g_im * u_re)
            return q_re, q_im

        total = lax.fori_loop(0, 8, station, total)
    q_re, q_im = total
    lane = lax.broadcasted_iota(jnp.int32, (PACKED, LANES), 1)
    image = jnp.zeros((PACKED, LANES), f32)
    for w in range(WINDOWS):
        column = jnp.sum(cos_ref[w] * q_re - sin_ref[w] * q_im, axis=1, keepdims=True)
        for q in range(4):
            image = jnp.where(lane == q * WINDOWS + w, column[q * PACKED : (q + 1) * PACKED], image)
    used = lax.broadcasted_iota(jnp.int32, (16, 8, LANES), 1) < PARTS
    u = jnp.where(used, u_ref[...], 0.0)
    ss = jnp.sum(jnp.sum(u * u, axis=0), axis=0, keepdims=True)
    for d in range(16):
        buf_ref[d, :PACKED, :] = image
        buf_ref[d, PACKED:, :] = jnp.broadcast_to(ss, (IMAGE - PACKED, LANES))


def first_adjoint(idx_ref, own_ref, oth_ref, cos_ref, sin_ref, buf_ref, u_ref):
    c = idx_ref[2]
    for ref, core in ((own_ref, c), (oth_ref, 1 - c)):
        for s in range(8):
            terms = [ref[s, GREEN_ROWS + 8 * t : GREEN_ROWS + 8 * t + 8, :].astype(f32) for t in range(3)]
            u_ref[core * 8 + s] = (terms[0] + terms[1]) + terms[2]
    data_to_model(c, u_ref, own_ref, oth_ref, cos_ref, sin_ref, buf_ref)


def norm_of(row):
    return jnp.broadcast_to(jnp.sqrt(jnp.sum(row, axis=1, keepdims=True)), (1, LANES))


def next_adjoint(idx_ref, own_ref, oth_ref, cos_ref, sin_ref, d0, d1, d2, d3, left_ref, right_ref, buf_ref, u_ref):
    c = idx_ref[2]
    data = (d0[...] + d1[...]) + (d2[...] + d3[...])
    alpha = norm_of(data[0, SQUARES : SQUARES + 1])
    beta = right_ref[PACKED : PACKED + 1]
    u_ref[...] = data / alpha[None] - alpha[None] * (left_ref[...] / beta[None])
    u_ref[0, SQUARES : SQUARES + 1, :] = alpha
    data_to_model(c, u_ref, own_ref, oth_ref, cos_ref, sin_ref, buf_ref)


def new_right(image_ref, right_ref, prev_ref, left_ref):
    image = jnp.sum(image_ref[...], axis=0)
    beta = norm_of(image[PACKED : PACKED + 1])
    right = image[:PACKED] / beta
    if prev_ref is not None:
        right = right - beta * (prev_ref[:PACKED] / left_ref[0, SQUARES : SQUARES + 1])
    right_ref[:PACKED] = right
    right_ref[PACKED:] = jnp.broadcast_to(beta, (IMAGE - PACKED, LANES))
    return right, jnp.sum(right * right, axis=0, keepdims=True)


def forward(first, idx_ref, own_ref, oth_ref, cos_ref, sin_ref, image_ref, *refs):
    prev_ref, left_ref, data_ref, right_ref, spec = ((None, None) + refs) if first else refs
    right, ss = new_right(image_ref, right_ref, prev_ref, left_ref)
    model_to_data(right, ss, idx_ref[2], own_ref, oth_ref, cos_ref, sin_ref, data_ref, spec)


def last_right(image_ref, prev_ref, left_ref, right_ref, ss_ref):
    right, ss = new_right(image_ref, right_ref, prev_ref, left_ref)
    ss_ref[...] = jnp.broadcast_to(ss, (8, LANES))


def finish(idx_ref, s0, s1, s2, s3, v0_ref, v1_ref, v2_ref, u1_ref, u2_ref, half_ref, slip_ref, direction_ref, misfit_ref, scale):
    x, zl, c, win = idx_ref[0], idx_ref[1], idx_ref[2], idx_ref[3]
    squares = (s0[...] + s1[...]) + (s2[...] + s3[...])
    at = slice(PACKED, PACKED + 1)
    alphas = [u1_ref[0, SQUARES : SQUARES + 1], u2_ref[0, SQUARES : SQUARES + 1], norm_of(squares[0:1])]
    betas = [v0_ref[at], v1_ref[at], v2_ref[at]]
    rights = [ref[:PACKED] / a for ref, a in zip((v0_ref, v1_ref, v2_ref), alphas)]
    phi_bar, rho_bar = betas[0], alphas[0]
    search, estimate = rights[0], jnp.zeros((PACKED, LANES), f32)
    for alpha, beta, right in zip(alphas[1:], betas[1:], rights[1:]):
        rho = jnp.sqrt(rho_bar * rho_bar + beta * beta)
        cosine, sine = rho_bar / rho, beta / rho
        theta = sine * alpha
        rho_bar = -cosine * alpha
        phi = cosine * phi_bar
        phi_bar = sine * phi_bar
        estimate = estimate + phi / rho * search
        search = right - theta / rho * search
    for value, ref in ((estimate, slip_ref), (search * scale, direction_ref)):
        for h in range(2):
            left = (2 * zl + h) * WINDOWS + win * 4
            ref[h * PACKED : (h + 1) * PACKED, :] = pltpu.roll(value, LANES - left, 1)[:, :4]
    own = u2_ref[c * 8 + x * 2 + zl]
    other = half_ref[...]
    for comp in range(COMP):
        rows = slice(2 * comp, 2 * comp + 2)
        for h in range(2):
            value = jnp.where(zl == h, own[rows], other[rows])
            misfit_ref[0, comp, :, h * LANES : (h + 1) * LANES] = value / betas[2] * phi_bar


def shifted(array):
    return [lax.ppermute(array, X, [(i, (i + k) % 4) for i in range(4)]) for k in (1, 2, 3)]


def summed_over_patches(array):
    both = array + lax.ppermute(array, C, [(0, 1), (1, 0)])
    return [both, *shifted(both)]


def summed_over_frequencies(buf):
    return lax.all_to_all(buf, (ZL, Y, ZH), 0, 0, tiled=True)


def local(green, records, onsets, mask):
    x, zl, c, win = (lax.axis_index(a) for a in (X, ZL, C, WIN))
    idx = jnp.stack([x, zl, c, win]).astype(jnp.int32)
    packed = pack(mask, green, records).reshape(8, 2 * ROWS, LANES)
    arrived = lax.all_to_all(packed, (X, ZL), 0, 0, tiled=True).reshape(8, 2, ROWS, LANES)
    sent = jnp.broadcast_to(onsets.reshape(1, 1, 128), (16, 1, 128))
    onset_rows = lax.all_to_all(sent, (ZL, Y, ZH), 0, 0, tiled=True)
    onset_rows = onset_rows.reshape(2, 8, 32, 4).transpose(0, 2, 1, 3).reshape(PATCHES, WINDOWS)
    table = ((WINDOWS, PATCHES, LANES), f32)
    cosine, sine = call(table_body, [table, table], idx, onset_rows)
    own = lax.dynamic_index_in_dim(arrived, c, 1, keepdims=False)
    give = lax.dynamic_index_in_dim(arrived, 1 - c, 1, keepdims=False)
    oth = lax.ppermute(give, C, [(0, 1), (1, 0)])
    base = (idx, own, oth, cosine, sine)

    buf_shape, data_shape, right_shape = ((16, IMAGE, LANES), f32), ((16, 8, LANES), f32), ((IMAGE, LANES), f32)

    def forward_call(first, *args):
        return pl.pallas_call(
            functools.partial(forward, first),
            in_specs=[SMEM] + [VMEM] * (len(args) - 1),
            out_specs=[VMEM] * 2,
            out_shape=[jax.ShapeDtypeStruct(*data_shape), jax.ShapeDtypeStruct(*right_shape)],
            scratch_shapes=[pltpu.VMEM((2, PATCHES, LANES), f32)],
            compiler_params=PARAMS,
            cost_estimate=pl.CostEstimate(flops=2_000_000, bytes_accessed=4_000_000, transcendentals=0),
        )(*args)

    buf, u0 = call(first_adjoint, [buf_shape, data_shape], *base)
    data, v0 = forward_call(True, *base, summed_over_frequencies(buf))
    buf, u1 = call(next_adjoint, [buf_shape, data_shape], *base, *summed_over_patches(data), u0, v0)
    data, v1 = forward_call(False, *base, summed_over_frequencies(buf), v0, u1)
    buf, u2 = call(next_adjoint, [buf_shape, data_shape], *base, *summed_over_patches(data), u1, v1)
    give = lax.dynamic_index_in_dim(u2, c * 8 + x * 2 + (1 - zl), 0, keepdims=False)
    half = lax.ppermute(give, ZL, [(0, 1), (1, 0)])
    v2, ss = call(last_right, [right_shape, ((8, LANES), f32)], summed_over_frequencies(buf), v1, u2)
    scale = math.sqrt(512 * 32)
    return call(
        functools.partial(finish, scale=scale),
        [((32, 4), f32), ((32, 4), f32), ((1, COMP, 2, 256), f32)],
        idx, *summed_over_patches(ss), v0, v1, v2, u1, u2, half,
    )


def solution(mesh):
    finer = Mesh(mesh.devices.reshape(4, 2, 2, 4, 2), (X, ZL, C, Y, ZH))
    return jax.shard_map(
        local,
        mesh=finer,
        in_specs=(P(STA, None, None, None, WIN), P(STA, None, None, WIN), P(STA, WIN), P(STA, None)),
        out_specs=(P(STA, WIN), P(STA, WIN), P(STA, None, None, WIN)),
        check_vma=False,
    )
```

```python
import functools
import math

import jax
import jax.numpy as jnp
from jax import lax
from jax.experimental import pallas as pl
from jax.experimental.pallas import tpu as pltpu
from jax.sharding import Mesh
from jax.sharding import PartitionSpec as P

X, ZL, C, Y, ZH = "x", "zl", "core", "y", "zh"
STA = (X, ZL, C)
WIN = (Y, ZH)
SAMPLES = 4096
LANES = 128
COMP = 3
PARTS = 2 * COMP
PATCHES = 64
WINDOWS = 32
GREEN_ROWS = PARTS * PATCHES
TERMS = 2
ROWS = GREEN_ROWS + 8 * TERMS
PACKED = 16
IMAGE = 24
SQUARES = 6
f32, bf16 = jnp.float32, jnp.bfloat16
VMEM = pl.BlockSpec(memory_space=pltpu.VMEM)
HBM = pl.BlockSpec(memory_space=pltpu.HBM)
SMEM = pl.BlockSpec(memory_space=pltpu.SMEM)
PARAMS = pltpu.CompilerParams(vmem_limit_bytes=16 << 20)


def call(body, outs, *args, flops=2_000_000):
    return pl.pallas_call(
        body,
        in_specs=[SMEM if a.dtype == jnp.int32 and a.ndim == 1 else VMEM for a in args],
        out_specs=[VMEM] * len(outs),
        out_shape=[jax.ShapeDtypeStruct(s, d) for s, d in outs],
        compiler_params=PARAMS,
        cost_estimate=pl.CostEstimate(flops=flops, bytes_accessed=4_000_000, transcendentals=0),
    )(*args)


def pack_body(mask_hbm, green_hbm, rec_hbm, out_hbm, mask_ref, green_ref, rec_ref, out_ref, rows, in_sems, out_sems):
    reads = [pltpu.make_async_copy(green_hbm.at[0, k // 2, k % 2], green_ref.at[k], in_sems.at[k]) for k in range(PARTS)]
    reads.append(pltpu.make_async_copy(rec_hbm.at[0], rec_ref, in_sems.at[PARTS]))
    reads.append(pltpu.make_async_copy(mask_hbm, mask_ref, in_sems.at[PARTS + 1]))
    for read in reversed(reads):
        read.start()
    reads[PARTS + 1].wait()
    reads[PARTS].wait()
    rows[...] = jnp.zeros_like(rows)
    for comp in range(COMP):
        rows[2 * comp : 2 * comp + 2, :] = jnp.where(mask_ref[0, comp] != 0, rec_ref[comp], 0.0)
    for half in range(2):
        rest = rows[:, half * LANES : (half + 1) * LANES]
        for term in range(TERMS):
            piece = rest.astype(bf16)
            rest = rest - piece.astype(f32)
            at = GREEN_ROWS + 8 * term
            for x in range(4):
                for c in range(2):
                    out_ref[x, half, c, at : at + 8, :] = piece
    writes = []
    for k in range(PARTS + 1):
        if k < PARTS:
            used = mask_ref[0, k // 2] != 0
            reads[k].wait()
            for x in range(4):
                for zl in range(2):
                    for c in range(2):
                        at = x * 128 + zl * 64 + c * 32
                        block = green_ref[k, at : at + 32, :]
                        block = jnp.where(used, block, jnp.zeros_like(block))
                        to = k * PATCHES + zl * 32
                        for half in range(2):
                            out_ref[x, half, c, to : to + 32, :] = block[:, half * LANES : (half + 1) * LANES]
        span = pl.ds(k * PATCHES, PATCHES if k < PARTS else 8 * TERMS)
        write = pltpu.make_async_copy(out_ref.at[:, :, :, span], out_hbm.at[:, :, :, span], out_sems.at[k])
        write.start()
        writes.append(write)
    for write in writes:
        write.wait()


def pack(mask, green, records):
    held = (4, 2, 2, ROWS, LANES)
    return pl.pallas_call(
        pack_body,
        in_specs=[HBM] * 3,
        out_specs=HBM,
        out_shape=jax.ShapeDtypeStruct(held, bf16),
        scratch_shapes=[
            pltpu.SMEM((1, COMP), jnp.int32),
            pltpu.VMEM((PARTS, 512, 256), bf16),
            pltpu.VMEM((COMP, 2, 256), f32),
            pltpu.VMEM(held, bf16),
            pltpu.VMEM((8, 256), f32),
            pltpu.SemaphoreType.DMA((PARTS + 2,)),
            pltpu.SemaphoreType.DMA((PARTS + 1,)),
        ],
        cost_estimate=pl.CostEstimate(flops=4_000_000, bytes_accessed=4_000_000, transcendentals=0),
    )(mask, green, records)


def table_body(idx_ref, o0, o1, o2, o3, cos_ref, sin_ref):
    y, z = idx_ref[3] // 2, (idx_ref[3] % 2) * 2 + idx_ref[1]
    first = idx_ref[3] * 256 + idx_ref[1] * LANES
    freq = lax.broadcasted_iota(jnp.int32, (32, LANES), 1) + first
    for ky, ref in enumerate((o0, o1, o2, o3)):
        for kz in range(4):
            y_from, z_from = (y - ky) & 3, (z - kz) & 3
            window = (y_from * 2 + z_from // 2) * 4
            patch = pl.multiple_of((z_from % 2) * 32, 32)
            columns = jnp.transpose(ref[kz], (1, 0))
            for j in range(4):
                onset = jnp.broadcast_to(columns[:, j : j + 1], (32, LANES))
                turns = onset * freq + SAMPLES // 8
                quarter = lax.shift_right_logical(turns, 10) & 3
                angle = ((turns & (SAMPLES // 4 - 1)) - SAMPLES // 8).astype(f32) * (2.0 * math.pi / SAMPLES)
                t = angle * angle
                s = angle * (1.0 + t * (-1 / 6 + t * (1 / 120 + t * (-1 / 5040 + t * (1 / 362880)))))
                c = 1.0 + t * (-0.5 + t * (1 / 24 + t * (-1 / 720 + t * (1 / 40320 + t * (-1 / 3628800)))))
                odd = (quarter & 1) == 1
                cosine = jnp.where(odd, s, c)
                sine = jnp.where(odd, c, s)
                cos_ref[window + j, pl.ds(patch, 32), :] = jnp.where((quarter == 1) | (quarter == 2), -cosine, cosine)
                sin_ref[window + j, pl.ds(patch, 32), :] = jnp.where(quarter >= 2, -sine, sine)


def model_to_data(model, ss, c, own_ref, oth_ref, cos_ref, sin_ref, data_ref, spec):
    for q in range(4):
        re = jnp.zeros((PACKED, LANES), f32)
        im = jnp.zeros((PACKED, LANES), f32)
        for w in range(WINDOWS):
            at = q * WINDOWS + w
            v = jnp.broadcast_to(model[:, at : at + 1], (PACKED, LANES))
            re = re + v * cos_ref[w, q * PACKED : (q + 1) * PACKED, :]
            im = im - v * sin_ref[w, q * PACKED : (q + 1) * PACKED, :]
        spec[0, q * PACKED : (q + 1) * PACKED, :] = re
        spec[1, q * PACKED : (q + 1) * PACKED, :] = im
    re, im = spec[0], spec[1]
    zero = jnp.zeros((2, LANES), f32)
    for ref, core in ((own_ref, c), (oth_ref, 1 - c)):

        def station(s, carry, ref=ref, core=core):
            for comp in range(COMP):
                at = 2 * comp * PATCHES
                g_re = ref[s, at : at + PATCHES, :].astype(f32)
                g_im = ref[s, at + PATCHES : at + 2 * PATCHES, :].astype(f32)
                data_ref[core * 8 + s, 2 * comp : 2 * comp + 1, :] = jnp.sum(g_re * re - g_im * im, axis=0, keepdims=True)
                data_ref[core * 8 + s, 2 * comp + 1 : 2 * comp + 2, :] = jnp.sum(g_re * im + g_im * re, axis=0, keepdims=True)
            data_ref[core * 8 + s, SQUARES:, :] = zero
            return carry

        lax.fori_loop(0, 8, station, 0)
    data_ref[0, SQUARES : SQUARES + 1, :] = ss


def data_to_model(c, u_ref, own_ref, oth_ref, cos_ref, sin_ref, buf_ref):
    total = (jnp.zeros((PATCHES, LANES), f32), jnp.zeros((PATCHES, LANES), f32))
    for ref, core in ((own_ref, c), (oth_ref, 1 - c)):

        def station(s, carry, ref=ref, core=core):
            q_re, q_im = carry
            for comp in range(COMP):
                at = 2 * comp * PATCHES
                g_re = ref[s, at : at + PATCHES, :].astype(f32)
                g_im = ref[s, at + PATCHES : at + 2 * PATCHES, :].astype(f32)
                u_re = u_ref[core * 8 + s, 2 * comp : 2 * comp + 1, :]
                u_im = u_ref[core * 8 + s, 2 * comp + 1 : 2 * comp + 2, :]
                q_re = q_re + (g_re * u_re + g_im * u_im)
                q_im = q_im + (g_re * u_im - g_im * u_re)
            return q_re, q_im

        total = lax.fori_loop(0, 8, station, total)
    q_re, q_im = total
    lane = lax.broadcasted_iota(jnp.int32, (PACKED, LANES), 1)
    image = jnp.zeros((PACKED, LANES), f32)
    for w in range(WINDOWS):
        column = jnp.sum(cos_ref[w] * q_re - sin_ref[w] * q_im, axis=1, keepdims=True)
        for q in range(4):
            image = jnp.where(lane == q * WINDOWS + w, column[q * PACKED : (q + 1) * PACKED], image)
    used = lax.broadcasted_iota(jnp.int32, (16, 8, LANES), 1) < PARTS
    u = jnp.where(used, u_ref[...], 0.0)
    ss = jnp.sum(jnp.sum(u * u, axis=0), axis=0, keepdims=True)
    for d in range(16):
        buf_ref[d, :PACKED, :] = image
        buf_ref[d, PACKED:, :] = jnp.broadcast_to(ss, (IMAGE - PACKED, LANES))


def first_adjoint(idx_ref, own_ref, oth_ref, cos_ref, sin_ref, buf_ref, u_ref):
    c = idx_ref[2]
    for ref, core in ((own_ref, c), (oth_ref, 1 - c)):
        for s in range(8):
            terms = [ref[s, GREEN_ROWS + 8 * t : GREEN_ROWS + 8 * t + 8, :].astype(f32) for t in range(TERMS)]
            u_ref[core * 8 + s] = sum(terms)
    data_to_model(c, u_ref, own_ref, oth_ref, cos_ref, sin_ref, buf_ref)


def norm_of(row):
    return jnp.broadcast_to(jnp.sqrt(jnp.sum(row, axis=1, keepdims=True)), (1, LANES))


def next_adjoint(idx_ref, own_ref, oth_ref, cos_ref, sin_ref, d0, d1, d2, d3, left_ref, right_ref, buf_ref, u_ref):
    c = idx_ref[2]
    data = (d0[...] + d1[...]) + (d2[...] + d3[...])
    alpha = norm_of(data[0, SQUARES : SQUARES + 1])
    beta = right_ref[PACKED : PACKED + 1]
    u_ref[...] = data / alpha[None] - alpha[None] * (left_ref[...] / beta[None])
    u_ref[0, SQUARES : SQUARES + 1, :] = alpha
    data_to_model(c, u_ref, own_ref, oth_ref, cos_ref, sin_ref, buf_ref)


def new_right(image_ref, right_ref, prev_ref, left_ref):
    image = jnp.sum(image_ref[...], axis=0)
    beta = norm_of(image[PACKED : PACKED + 1])
    right = image[:PACKED] / beta
    if prev_ref is not None:
        right = right - beta * (prev_ref[:PACKED] / left_ref[0, SQUARES : SQUARES + 1])
    right_ref[:PACKED] = right
    right_ref[PACKED:] = jnp.broadcast_to(beta, (IMAGE - PACKED, LANES))
    return right, jnp.sum(right * right, axis=0, keepdims=True)


def forward(first, idx_ref, own_ref, oth_ref, cos_ref, sin_ref, image_ref, *refs):
    prev_ref, left_ref, data_ref, right_ref, spec = ((None, None) + refs) if first else refs
    right, ss = new_right(image_ref, right_ref, prev_ref, left_ref)
    model_to_data(right, ss, idx_ref[2], own_ref, oth_ref, cos_ref, sin_ref, data_ref, spec)


def last_right(idx_ref, image_ref, prev_ref, left_ref, right_ref, ss_ref, give_ref):
    right, ss = new_right(image_ref, right_ref, prev_ref, left_ref)
    ss_ref[...] = jnp.broadcast_to(ss, (8, LANES))
    give_ref[...] = left_ref[idx_ref[2] * 8 + idx_ref[0] * 2 + (1 - idx_ref[1])]


def finish(idx_ref, s0, s1, s2, s3, v0_ref, v1_ref, v2_ref, u1_ref, u2_ref, half_ref, slip_ref, direction_ref, misfit_ref, scale):
    x, zl, c, win = idx_ref[0], idx_ref[1], idx_ref[2], idx_ref[3]
    squares = (s0[...] + s1[...]) + (s2[...] + s3[...])
    at = slice(PACKED, PACKED + 1)
    alphas = [u1_ref[0, SQUARES : SQUARES + 1], u2_ref[0, SQUARES : SQUARES + 1], norm_of(squares[0:1])]
    betas = [v0_ref[at], v1_ref[at], v2_ref[at]]
    rights = [ref[:PACKED] / a for ref, a in zip((v0_ref, v1_ref, v2_ref), alphas)]
    phi_bar, rho_bar = betas[0], alphas[0]
    search, estimate = rights[0], jnp.zeros((PACKED, LANES), f32)
    for alpha, beta, right in zip(alphas[1:], betas[1:], rights[1:]):
        rho = jnp.sqrt(rho_bar * rho_bar + beta * beta)
        cosine, sine = rho_bar / rho, beta / rho
        theta = sine * alpha
        rho_bar = -cosine * alpha
        phi = cosine * phi_bar
        phi_bar = sine * phi_bar
        estimate = estimate + phi / rho * search
        search = right - theta / rho * search
    for value, ref in ((estimate, slip_ref), (search * scale, direction_ref)):
        for h in range(2):
            left = (2 * zl + h) * WINDOWS + win * 4
            rolled = pltpu.roll(value, LANES - left, 1)
            ref[:, h * PACKED : (h + 1) * PACKED] = jnp.transpose(rolled, (1, 0))[:4]
    own = u2_ref[c * 8 + x * 2 + zl]
    other = half_ref[...]
    for comp in range(COMP):
        rows = slice(2 * comp, 2 * comp + 2)
        for h in range(2):
            value = jnp.where(zl == h, own[rows], other[rows])
            misfit_ref[0, comp, :, h * LANES : (h + 1) * LANES] = value / betas[2] * phi_bar


def rotated(array, axis, at=range(4)):
    return [lax.ppermute(array, axis, [(at[i], at[(i + k) % 4]) for i in range(4)]) for k in (1, 2, 3)]


def summed_over_patches(array):
    both = array + lax.ppermute(array, C, [(0, 1), (1, 0)])
    return [both, *rotated(both, X)]


def summed_over_frequencies(buf):
    return lax.all_to_all(buf, (ZL, Y, ZH), 0, 0, tiled=True)


def local(green, records, onsets, mask):
    x, zl, c, win = (lax.axis_index(a) for a in (X, ZL, C, WIN))
    idx = jnp.stack([x, zl, c, win]).astype(jnp.int32)
    onset_rows = onsets.T[None]
    rows = jnp.concatenate([onset_rows, *rotated(onset_rows, (ZL, ZH), (0, 2, 1, 3))], axis=0)
    packed = pack(mask, green, records).reshape(8, 2 * ROWS, LANES)
    packed, rows, idx = lax.optimization_barrier((packed, rows, idx))
    arrived = lax.all_to_all(packed, (X, ZL), 0, 0, tiled=True)
    turned = rotated(rows, Y)
    arrived, rows, idx, *turned = lax.optimization_barrier((arrived, rows, idx, *turned))
    arrived = arrived.reshape(8, 2, ROWS, LANES)
    table = ((WINDOWS, PATCHES, LANES), f32)
    cosine, sine = call(table_body, [table, table], idx, rows, *turned)
    own = lax.dynamic_index_in_dim(arrived, c, 1, keepdims=False)
    give = lax.dynamic_index_in_dim(arrived, 1 - c, 1, keepdims=False)
    oth = lax.ppermute(give, C, [(0, 1), (1, 0)])
    base = (idx, own, oth, cosine, sine)

    buf_shape, data_shape, right_shape = ((16, IMAGE, LANES), f32), ((16, 8, LANES), f32), ((IMAGE, LANES), f32)

    def forward_call(first, *args):
        return pl.pallas_call(
            functools.partial(forward, first),
            in_specs=[SMEM] + [VMEM] * (len(args) - 1),
            out_specs=[VMEM] * 2,
            out_shape=[jax.ShapeDtypeStruct(*data_shape), jax.ShapeDtypeStruct(*right_shape)],
            scratch_shapes=[pltpu.VMEM((2, PATCHES, LANES), f32)],
            compiler_params=PARAMS,
            cost_estimate=pl.CostEstimate(flops=2_000_000, bytes_accessed=4_000_000, transcendentals=0),
        )(*args)

    buf, u0 = call(first_adjoint, [buf_shape, data_shape], *base)
    data, v0 = forward_call(True, *base, summed_over_frequencies(buf))
    buf, u1 = call(next_adjoint, [buf_shape, data_shape], *base, *summed_over_patches(data), u0, v0)
    data, v1 = forward_call(False, *base, summed_over_frequencies(buf), v0, u1)
    buf, u2 = call(next_adjoint, [buf_shape, data_shape], *base, *summed_over_patches(data), u1, v1)
    tile = ((8, LANES), f32)
    v2, ss, give = call(last_right, [right_shape, tile, tile], idx, summed_over_frequencies(buf), v1, u2)
    half = lax.ppermute(give, ZL, [(0, 1), (1, 0)])
    scale = math.sqrt(512 * 32)
    slip, direction, misfit = call(
        functools.partial(finish, scale=scale),
        [((4, 32), f32), ((4, 32), f32), ((1, COMP, 2, 256), f32)],
        idx, *summed_over_patches(ss), v0, v1, v2, u1, u2, half,
    )
    return slip.T, direction.T, misfit


def solution(mesh):
    finer = Mesh(mesh.devices.reshape(4, 2, 2, 4, 2), (X, ZL, C, Y, ZH))
    return jax.shard_map(
        local,
        mesh=finer,
        in_specs=(P(STA, None, None, None, WIN), P(STA, None, None, WIN), P(STA, WIN), P(STA, None)),
        out_specs=(P(STA, WIN), P(STA, WIN), P(STA, None, None, WIN)),
        check_vma=False,
    )
```

```python
import functools
import math

import jax
import jax.numpy as jnp
from jax import lax
from jax.experimental import pallas as pl
from jax.experimental.pallas import tpu as pltpu
from jax.sharding import Mesh
from jax.sharding import PartitionSpec as P

X, ZL, C, Y, ZH = "x", "zl", "core", "y", "zh"
STA = (X, ZL, C)
WIN = (Y, ZH)
SAMPLES = 4096
LANES = 128
COMP = 3
PARTS = 2 * COMP
PATCHES = 64
WINDOWS = 32
GREEN_ROWS = PARTS * PATCHES
TERMS = 2
ROWS = GREEN_ROWS + 8 * TERMS
PACKED = 16
IMAGE = 24
SQUARES = 6
f32, bf16 = jnp.float32, jnp.bfloat16
VMEM = pl.BlockSpec(memory_space=pltpu.VMEM)
HBM = pl.BlockSpec(memory_space=pltpu.HBM)
UNROLL = 4
ORDER = (3, 1, 2)
SPLIT = 24
PARAMS = pltpu.CompilerParams(vmem_limit_bytes=16 << 20)


def call(body, outs, *args, flops=2_000_000):
    return pl.pallas_call(
        body,
        in_specs=[VMEM] * len(args),
        out_specs=[VMEM] * len(outs),
        out_shape=[jax.ShapeDtypeStruct(s, d) for s, d in outs],
        compiler_params=PARAMS,
        cost_estimate=pl.CostEstimate(flops=flops, bytes_accessed=4_000_000, transcendentals=0),
    )(*args)


def pack_body(mask_hbm, green_hbm, rec_hbm, out_hbm, mask_ref, green_ref, rec_ref, out_ref, rows, in_sems, out_sems):
    reads = [pltpu.make_async_copy(green_hbm.at[0, k // 2, k % 2], green_ref.at[k], in_sems.at[k]) for k in range(PARTS)]
    reads.append(pltpu.make_async_copy(rec_hbm.at[0], rec_ref, in_sems.at[PARTS]))
    reads.append(pltpu.make_async_copy(mask_hbm, mask_ref, in_sems.at[PARTS + 1]))
    for read in reversed(reads):
        read.start()
    reads[PARTS + 1].wait()
    reads[PARTS].wait()
    rows[...] = jnp.zeros_like(rows)
    for comp in range(COMP):
        rows[2 * comp : 2 * comp + 2, :] = jnp.where(mask_ref[0, comp] != 0, rec_ref[comp], 0.0)
    for half in range(2):
        rest = rows[:, half * LANES : (half + 1) * LANES]
        for term in range(TERMS):
            piece = rest.astype(bf16)
            rest = rest - piece.astype(f32)
            at = GREEN_ROWS + 8 * term
            for x in range(4):
                for c in range(2):
                    out_ref[x, half, c, at : at + 8, :] = piece
    writes = []
    for k in range(PARTS + 1):
        if k < PARTS:
            used = mask_ref[0, k // 2] != 0
            reads[k].wait()
            for x in range(4):
                for zl in range(2):
                    for c in range(2):
                        at = x * 128 + zl * 64 + c * 32
                        block = green_ref[k, at : at + 32, :]
                        block = jnp.where(used, block, jnp.zeros_like(block))
                        to = k * PATCHES + zl * 32
                        for half in range(2):
                            out_ref[x, half, c, to : to + 32, :] = block[:, half * LANES : (half + 1) * LANES]
        span = pl.ds(k * PATCHES, PATCHES if k < PARTS else 8 * TERMS)
        write = pltpu.make_async_copy(out_ref.at[:, :, :, span], out_hbm.at[:, :, :, span], out_sems.at[k])
        write.start()
        writes.append(write)
    for write in writes:
        write.wait()


def pack(mask, green, records):
    held = (4, 2, 2, ROWS, LANES)
    return pl.pallas_call(
        pack_body,
        in_specs=[HBM] * 3,
        out_specs=HBM,
        out_shape=jax.ShapeDtypeStruct(held, bf16),
        scratch_shapes=[
            pltpu.SMEM((1, COMP), jnp.int32),
            pltpu.VMEM((PARTS, 512, 256), bf16),
            pltpu.VMEM((COMP, 2, 256), f32),
            pltpu.VMEM(held, bf16),
            pltpu.VMEM((8, 256), f32),
            pltpu.SemaphoreType.DMA((PARTS + 2,)),
            pltpu.SemaphoreType.DMA((PARTS + 1,)),
        ],
        cost_estimate=pl.CostEstimate(flops=4_000_000, bytes_accessed=4_000_000, transcendentals=0),
    )(mask, green, records)


def fill_tables(onset_ref, places, cos_ref, sin_ref):
    y, z = lax.axis_index(Y), lax.axis_index(ZH) * 2 + lax.axis_index(ZL)
    first = lax.axis_index(WIN) * 256 + lax.axis_index(ZL) * LANES
    freq = lax.broadcasted_iota(jnp.int32, (32, LANES), 1) + first
    for y_from in places:
        for z_from in range(4):
            window = ((y_from - places[0]) * 2 + z_from // 2) * 4
            patch = slice(z_from % 2 * 32, z_from % 2 * 32 + 32)
            columns = jnp.transpose(onset_ref[y ^ y_from, z ^ z_from], (1, 0))
            for j in range(4):
                onset = jnp.broadcast_to(columns[:, j : j + 1], (32, LANES))
                turns = onset * freq + SAMPLES // 8
                quarter = lax.shift_right_logical(turns, 10) & 3
                angle = ((turns & (SAMPLES // 4 - 1)) - SAMPLES // 8).astype(f32) * (2.0 * math.pi / SAMPLES)
                t = angle * angle
                s = angle * (1.0 + t * (-1 / 6 + t * (1 / 120 + t * (-1 / 5040 + t * (1 / 362880)))))
                c = 1.0 + t * (-0.5 + t * (1 / 24 + t * (-1 / 720 + t * (1 / 40320 + t * (-1 / 3628800)))))
                odd = (quarter & 1) == 1
                cosine = jnp.where(odd, s, c)
                sine = jnp.where(odd, c, s)
                cos_ref[window + j, patch, :] = jnp.where((quarter == 1) | (quarter == 2), -cosine, cosine)
                sin_ref[window + j, patch, :] = jnp.where(quarter >= 2, -sine, sine)


def table_body(onset_ref, cos_ref, sin_ref):
    fill_tables(onset_ref, range(3), cos_ref, sin_ref)


def tables_of(refs):
    cos_a, sin_a, cos_b, sin_b = refs
    return lambda w, rows: (cos_a[w, rows, :], sin_a[w, rows, :]) if w < SPLIT else (cos_b[w - SPLIT, rows, :], sin_b[w - SPLIT, rows, :])


def model_to_data(model, ss, green_ref, tables, data_ref, spec):
    for q in range(4):
        re = jnp.zeros((PACKED, LANES), f32)
        im = jnp.zeros((PACKED, LANES), f32)
        for w in range(WINDOWS):
            at = q * WINDOWS + w
            v = jnp.broadcast_to(model[:, at : at + 1], (PACKED, LANES))
            cosine, sine = tables(w, slice(q * PACKED, (q + 1) * PACKED))
            re = re + v * cosine
            im = im - v * sine
        spec[0, q * PACKED : (q + 1) * PACKED, :] = re
        spec[1, q * PACKED : (q + 1) * PACKED, :] = im
    re, im = spec[0], spec[1]
    zero = jnp.zeros((2, LANES), f32)

    def station(s, carry):
        for comp in range(COMP):
            at = 2 * comp * PATCHES
            g_re = green_ref[s, at : at + PATCHES, :].astype(f32)
            g_im = green_ref[s, at + PATCHES : at + 2 * PATCHES, :].astype(f32)
            data_ref[s, 2 * comp : 2 * comp + 1, :] = jnp.sum(g_re * re - g_im * im, axis=0, keepdims=True)
            data_ref[s, 2 * comp + 1 : 2 * comp + 2, :] = jnp.sum(g_re * im + g_im * re, axis=0, keepdims=True)
        data_ref[s, SQUARES:, :] = zero
        return carry

    lax.fori_loop(0, 16, station, 0, unroll=UNROLL)
    data_ref[0, SQUARES : SQUARES + 1, :] = ss


def data_to_model(u_ref, green_ref, tables, buf_ref):
    def station(s, carry):
        q_re, q_im = carry
        for comp in range(COMP):
            at = 2 * comp * PATCHES
            g_re = green_ref[s, at : at + PATCHES, :].astype(f32)
            g_im = green_ref[s, at + PATCHES : at + 2 * PATCHES, :].astype(f32)
            u_re = u_ref[s, 2 * comp : 2 * comp + 1, :]
            u_im = u_ref[s, 2 * comp + 1 : 2 * comp + 2, :]
            q_re = q_re + (g_re * u_re + g_im * u_im)
            q_im = q_im + (g_re * u_im - g_im * u_re)
        return q_re, q_im

    zero = jnp.zeros((PATCHES, LANES), f32)
    q_re, q_im = lax.fori_loop(0, 16, station, (zero, zero), unroll=UNROLL)
    lane = lax.broadcasted_iota(jnp.int32, (PACKED, LANES), 1)
    image = jnp.zeros((PACKED, LANES), f32)
    for w in range(WINDOWS):
        cosine, sine = tables(w, slice(0, PATCHES))
        column = jnp.sum(cosine * q_re - sine * q_im, axis=1, keepdims=True)
        for q in range(4):
            image = jnp.where(lane == q * WINDOWS + w, column[q * PACKED : (q + 1) * PACKED], image)
    used = lax.broadcasted_iota(jnp.int32, (16, 8, LANES), 1) < PARTS
    u = jnp.where(used, u_ref[...], 0.0)
    ss = jnp.sum(jnp.sum(u * u, axis=0), axis=0, keepdims=True)
    for d in range(16):
        buf_ref[d, :PACKED, :] = image
        buf_ref[d, PACKED:, :] = jnp.broadcast_to(ss, (IMAGE - PACKED, LANES))


def first_adjoint(green_ref, cos_a, sin_a, onset_ref, buf_ref, u_ref, cos_b, sin_b):
    fill_tables(onset_ref, range(3, 4), cos_b, sin_b)
    for s in range(16):
        terms = [green_ref[s, GREEN_ROWS + 8 * t : GREEN_ROWS + 8 * t + 8, :].astype(f32) for t in range(TERMS)]
        u_ref[s] = sum(terms)
    data_to_model(u_ref, green_ref, tables_of((cos_a, sin_a, cos_b, sin_b)), buf_ref)


def norm_of(row):
    return jnp.broadcast_to(jnp.sqrt(jnp.sum(row, axis=1, keepdims=True)), (1, LANES))


def next_adjoint(green_ref, t0, t1, t2, t3, d0, d1, d2, d3, left_ref, right_ref, buf_ref, u_ref):
    data = (d0[...] + d1[...]) + (d2[...] + d3[...])
    alpha = norm_of(data[0, SQUARES : SQUARES + 1])
    beta = right_ref[PACKED : PACKED + 1]
    u_ref[...] = data / alpha[None] - alpha[None] * (left_ref[...] / beta[None])
    u_ref[0, SQUARES : SQUARES + 1, :] = alpha
    data_to_model(u_ref, green_ref, tables_of((t0, t1, t2, t3)), buf_ref)


def new_right(image_ref, right_ref, prev_ref, left_ref):
    image = jnp.sum(image_ref[...], axis=0)
    beta = norm_of(image[PACKED : PACKED + 1])
    right = image[:PACKED] / beta
    if prev_ref is not None:
        right = right - beta * (prev_ref[:PACKED] / left_ref[0, SQUARES : SQUARES + 1])
    right_ref[:PACKED] = right
    right_ref[PACKED:] = jnp.broadcast_to(beta, (IMAGE - PACKED, LANES))
    return right, jnp.sum(right * right, axis=0, keepdims=True)


def forward(first, green_ref, t0, t1, t2, t3, image_ref, *refs):
    prev_ref, left_ref, data_ref, right_ref, spec = ((None, None) + refs) if first else refs
    right, ss = new_right(image_ref, right_ref, prev_ref, left_ref)
    model_to_data(right, ss, green_ref, tables_of((t0, t1, t2, t3)), data_ref, spec)


def last_right(image_ref, prev_ref, left_ref, right_ref, ss_ref, give_ref):
    right, ss = new_right(image_ref, right_ref, prev_ref, left_ref)
    ss_ref[...] = jnp.broadcast_to(ss, (8, LANES))
    give_ref[...] = left_ref[lax.axis_index(STA) ^ 2]


def finish(s0, s1, s2, s3, v0_ref, v1_ref, v2_ref, u1_ref, u2_ref, half_ref, slip_ref, direction_ref, misfit_ref, scale):
    zl, win = lax.axis_index(ZL), lax.axis_index(WIN)
    squares = (s0[...] + s1[...]) + (s2[...] + s3[...])
    at = slice(PACKED, PACKED + 1)
    alphas = [u1_ref[0, SQUARES : SQUARES + 1], u2_ref[0, SQUARES : SQUARES + 1], norm_of(squares[0:1])]
    betas = [v0_ref[at], v1_ref[at], v2_ref[at]]
    rights = [ref[:PACKED] / a for ref, a in zip((v0_ref, v1_ref, v2_ref), alphas)]
    phi_bar, rho_bar = betas[0], alphas[0]
    search, estimate = rights[0], jnp.zeros((PACKED, LANES), f32)
    for alpha, beta, right in zip(alphas[1:], betas[1:], rights[1:]):
        rho = jnp.sqrt(rho_bar * rho_bar + beta * beta)
        cosine, sine = rho_bar / rho, beta / rho
        theta = sine * alpha
        rho_bar = -cosine * alpha
        phi = cosine * phi_bar
        phi_bar = sine * phi_bar
        estimate = estimate + phi / rho * search
        search = right - theta / rho * search
    for value, ref in ((estimate, slip_ref), (search * scale, direction_ref)):
        for h in range(2):
            left = (2 * zl + h) * WINDOWS + win * 4
            rolled = pltpu.roll(value, LANES - left, 1)
            ref[:, h * PACKED : (h + 1) * PACKED] = jnp.transpose(rolled, (1, 0))[:4]
    own = u2_ref[lax.axis_index(STA)]
    other = half_ref[...]
    for comp in range(COMP):
        rows = slice(2 * comp, 2 * comp + 2)
        for h in range(2):
            value = jnp.where(zl == h, own[rows], other[rows])
            misfit_ref[0, comp, :, h * LANES : (h + 1) * LANES] = value / betas[2] * phi_bar


def from_partners(array, axis, at=range(4)):
    held = {k: lax.ppermute(array, axis, [(at[i], at[i ^ k]) for i in range(4)]) for k in ORDER}
    return [held[k] for k in (1, 2, 3)]


def other_core(array):
    return lax.ppermute(array, C, [(0, 1), (1, 0)])


def summed_over_patches(array):
    both = array + other_core(array)
    side = lax.ppermute(both, (X, C), [(x * 2 + c, (x ^ (1, 3)[c]) * 2 + c) for x in range(4) for c in range(2)])
    across = lax.ppermute(both, X, [(x, x ^ 2) for x in range(4)])
    return [both, across, side, other_core(side)]


def summed_over_frequencies(buf):
    return lax.all_to_all(buf, (ZL, Y, ZH), 0, 0, tiled=True)


def local(green, records, onsets, mask):
    onset_rows = onsets.T[None]
    rows = jnp.concatenate([onset_rows, *from_partners(onset_rows, (ZL, ZH), (0, 2, 1, 3))], axis=0)
    packed = pack(mask, green, records).reshape(16, ROWS, LANES)
    packed, rows = lax.optimization_barrier((packed, rows))
    arrived = lax.all_to_all(packed, STA, 0, 0, tiled=True)
    gathered = jnp.stack([rows, *from_partners(rows, Y)])
    head, tail = ((SPLIT, PATCHES, LANES), f32), ((WINDOWS - SPLIT, PATCHES, LANES), f32)
    tables = call(table_body, [head, head], gathered)

    buf_shape, data_shape, right_shape = ((16, IMAGE, LANES), f32), ((16, 8, LANES), f32), ((IMAGE, LANES), f32)

    def forward_call(first, *args):
        return pl.pallas_call(
            functools.partial(forward, first),
            in_specs=[VMEM] * len(args),
            out_specs=[VMEM] * 2,
            out_shape=[jax.ShapeDtypeStruct(*data_shape), jax.ShapeDtypeStruct(*right_shape)],
            scratch_shapes=[pltpu.VMEM((2, PATCHES, LANES), f32)],
            compiler_params=PARAMS,
            cost_estimate=pl.CostEstimate(flops=2_000_000, bytes_accessed=4_000_000, transcendentals=0),
        )(*args)

    buf, u0, *rest = call(first_adjoint, [buf_shape, data_shape, tail, tail], arrived, *tables, gathered)
    base = (arrived, *tables, *rest)
    data, v0 = forward_call(True, *base, summed_over_frequencies(buf))
    buf, u1 = call(next_adjoint, [buf_shape, data_shape], *base, *summed_over_patches(data), u0, v0)
    data, v1 = forward_call(False, *base, summed_over_frequencies(buf), v0, u1)
    buf, u2 = call(next_adjoint, [buf_shape, data_shape], *base, *summed_over_patches(data), u1, v1)
    tile = ((8, LANES), f32)
    v2, ss, give = call(last_right, [right_shape, tile, tile], summed_over_frequencies(buf), v1, u2)
    half = lax.ppermute(give, ZL, [(0, 1), (1, 0)])
    scale = math.sqrt(512 * 32)
    slip, direction, misfit = call(
        functools.partial(finish, scale=scale),
        [((4, 32), f32), ((4, 32), f32), ((1, COMP, 2, 256), f32)],
        *summed_over_patches(ss), v0, v1, v2, u1, u2, half,
    )
    return slip.T, direction.T, misfit


def solution(mesh):
    finer = Mesh(mesh.devices.reshape(4, 2, 2, 4, 2), (X, ZL, C, Y, ZH))
    return jax.shard_map(
        local,
        mesh=finer,
        in_specs=(P(STA, None, None, None, WIN), P(STA, None, None, WIN), P(STA, WIN), P(STA, None)),
        out_specs=(P(STA, WIN), P(STA, WIN), P(STA, None, None, WIN)),
        check_vma=False,
    )
```

```python
import functools
import math

import jax
import jax.numpy as jnp
from jax import lax
from jax.experimental import pallas as pl
from jax.experimental.pallas import tpu as pltpu
from jax.sharding import Mesh
from jax.sharding import PartitionSpec as P

X, ZL, C, Y, ZH = "x", "zl", "core", "y", "zh"
STA = (X, ZL, C)
WIN = (Y, ZH)
SAMPLES = 4096
LANES = 128
COMP = 3
PARTS = 2 * COMP
PATCHES = 64
WINDOWS = 32
GREEN_ROWS = PARTS * PATCHES
TERMS = 2
ROWS = GREEN_ROWS + 8 * TERMS
PACKED = 16
IMAGE = 24
SQUARES = 6
f32, bf16 = jnp.float32, jnp.bfloat16
VMEM = pl.BlockSpec(memory_space=pltpu.VMEM)
HBM = pl.BlockSpec(memory_space=pltpu.HBM)
UNROLL = 4
ORDER = (3, 1, 2)
SPLIT = 24
PARAMS = pltpu.CompilerParams(vmem_limit_bytes=16 << 20)


def call(body, outs, *args, flops=2_000_000):
    return pl.pallas_call(
        body,
        in_specs=[VMEM] * len(args),
        out_specs=[VMEM] * len(outs),
        out_shape=[jax.ShapeDtypeStruct(s, d) for s, d in outs],
        compiler_params=PARAMS,
        cost_estimate=pl.CostEstimate(flops=flops, bytes_accessed=4_000_000, transcendentals=0),
    )(*args)


def pack_body(mask_hbm, green_hbm, rec_hbm, out_hbm, mask_ref, green_ref, rec_ref, out_ref, rows, in_sems, out_sems):
    reads = [pltpu.make_async_copy(green_hbm.at[0, k // 2, k % 2], green_ref.at[k], in_sems.at[k]) for k in range(PARTS)]
    reads.append(pltpu.make_async_copy(rec_hbm.at[0], rec_ref, in_sems.at[PARTS]))
    reads.append(pltpu.make_async_copy(mask_hbm, mask_ref, in_sems.at[PARTS + 1]))
    for read in reversed(reads):
        read.start()
    reads[PARTS + 1].wait()
    reads[PARTS].wait()
    rows[...] = jnp.zeros_like(rows)
    for comp in range(COMP):
        rows[2 * comp : 2 * comp + 2, :] = jnp.where(mask_ref[0, comp] != 0, rec_ref[comp], 0.0)
    for half in range(2):
        rest = rows[:, half * LANES : (half + 1) * LANES]
        for term in range(TERMS):
            piece = rest.astype(bf16)
            rest = rest - piece.astype(f32)
            at = GREEN_ROWS + 8 * term
            for x in range(4):
                for c in range(2):
                    out_ref[x, half, c, at : at + 8, :] = piece
    writes = []
    for k in range(PARTS + 1):
        if k < PARTS:
            used = mask_ref[0, k // 2] != 0
            reads[k].wait()
            for x in range(4):
                for zl in range(2):
                    for c in range(2):
                        at = x * 128 + zl * 64 + c * 32
                        block = green_ref[k, at : at + 32, :]
                        block = jnp.where(used, block, jnp.zeros_like(block))
                        to = k * PATCHES + zl * 32
                        for half in range(2):
                            out_ref[x, half, c, to : to + 32, :] = block[:, half * LANES : (half + 1) * LANES]
        span = pl.ds(k * PATCHES, PATCHES if k < PARTS else 8 * TERMS)
        write = pltpu.make_async_copy(out_ref.at[:, :, :, span], out_hbm.at[:, :, :, span], out_sems.at[k])
        write.start()
        writes.append(write)
    for write in writes:
        write.wait()


def pack(mask, green, records):
    held = (4, 2, 2, ROWS, LANES)
    return pl.pallas_call(
        pack_body,
        in_specs=[HBM] * 3,
        out_specs=HBM,
        out_shape=jax.ShapeDtypeStruct(held, bf16),
        scratch_shapes=[
            pltpu.SMEM((1, COMP), jnp.int32),
            pltpu.VMEM((PARTS, 512, 256), bf16),
            pltpu.VMEM((COMP, 2, 256), f32),
            pltpu.VMEM(held, bf16),
            pltpu.VMEM((8, 256), f32),
            pltpu.SemaphoreType.DMA((PARTS + 2,)),
            pltpu.SemaphoreType.DMA((PARTS + 1,)),
        ],
        cost_estimate=pl.CostEstimate(flops=4_000_000, bytes_accessed=4_000_000, transcendentals=0),
    )(mask, green, records)


def fill_tables(onset_ref, places, cos_ref, sin_ref):
    y, z = lax.axis_index(Y), lax.axis_index(ZH) * 2 + lax.axis_index(ZL)
    first = lax.axis_index(WIN) * 256 + lax.axis_index(ZL) * LANES
    freq = lax.broadcasted_iota(jnp.int32, (32, LANES), 1) + first
    for y_from in places:
        for z_from in range(4):
            window = ((y_from - places[0]) * 2 + z_from // 2) * 4
            patch = slice(z_from % 2 * 32, z_from % 2 * 32 + 32)
            columns = jnp.transpose(onset_ref[z ^ z_from, y ^ y_from], (1, 0))
            for j in range(4):
                onset = jnp.broadcast_to(columns[:, j : j + 1], (32, LANES))
                turns = onset * freq + SAMPLES // 8
                quarter = lax.shift_right_logical(turns, 10) & 3
                angle = ((turns & (SAMPLES // 4 - 1)) - SAMPLES // 8).astype(f32) * (2.0 * math.pi / SAMPLES)
                t = angle * angle
                s = angle * (1.0 + t * (-1 / 6 + t * (1 / 120 + t * (-1 / 5040 + t * (1 / 362880)))))
                c = 1.0 + t * (-0.5 + t * (1 / 24 + t * (-1 / 720 + t * (1 / 40320 + t * (-1 / 3628800)))))
                odd = (quarter & 1) == 1
                cosine = jnp.where(odd, s, c)
                sine = jnp.where(odd, c, s)
                cos_ref[window + j, patch, :] = jnp.where((quarter == 1) | (quarter == 2), -cosine, cosine)
                sin_ref[window + j, patch, :] = jnp.where(quarter >= 2, -sine, sine)


def table_body(onset_ref, cos_ref, sin_ref):
    fill_tables(onset_ref, range(3), cos_ref, sin_ref)


def tables_of(refs):
    cos_a, sin_a, cos_b, sin_b = refs
    return lambda w, rows: (cos_a[w, rows, :], sin_a[w, rows, :]) if w < SPLIT else (cos_b[w - SPLIT, rows, :], sin_b[w - SPLIT, rows, :])


def model_to_data(model, ss, green_ref, tables, data_ref, spec):
    for q in range(4):
        re = jnp.zeros((PACKED, LANES), f32)
        im = jnp.zeros((PACKED, LANES), f32)
        for w in range(WINDOWS):
            at = q * WINDOWS + w
            v = jnp.broadcast_to(model[:, at : at + 1], (PACKED, LANES))
            cosine, sine = tables(w, slice(q * PACKED, (q + 1) * PACKED))
            re = re + v * cosine
            im = im - v * sine
        spec[0, q * PACKED : (q + 1) * PACKED, :] = re
        spec[1, q * PACKED : (q + 1) * PACKED, :] = im
    re, im = spec[0], spec[1]
    zero = jnp.zeros((2, LANES), f32)

    def station(s, carry):
        for comp in range(COMP):
            at = 2 * comp * PATCHES
            g_re = green_ref[s, at : at + PATCHES, :].astype(f32)
            g_im = green_ref[s, at + PATCHES : at + 2 * PATCHES, :].astype(f32)
            data_ref[s, 2 * comp : 2 * comp + 1, :] = jnp.sum(g_re * re - g_im * im, axis=0, keepdims=True)
            data_ref[s, 2 * comp + 1 : 2 * comp + 2, :] = jnp.sum(g_re * im + g_im * re, axis=0, keepdims=True)
        data_ref[s, SQUARES:, :] = zero
        return carry

    lax.fori_loop(0, 16, station, 0, unroll=UNROLL)
    data_ref[0, SQUARES : SQUARES + 1, :] = ss


def data_to_model(u_ref, green_ref, tables, buf_ref):
    def station(s, carry):
        q_re, q_im = carry
        for comp in range(COMP):
            at = 2 * comp * PATCHES
            g_re = green_ref[s, at : at + PATCHES, :].astype(f32)
            g_im = green_ref[s, at + PATCHES : at + 2 * PATCHES, :].astype(f32)
            u_re = u_ref[s, 2 * comp : 2 * comp + 1, :]
            u_im = u_ref[s, 2 * comp + 1 : 2 * comp + 2, :]
            q_re = q_re + (g_re * u_re + g_im * u_im)
            q_im = q_im + (g_re * u_im - g_im * u_re)
        return q_re, q_im

    zero = jnp.zeros((PATCHES, LANES), f32)
    q_re, q_im = lax.fori_loop(0, 16, station, (zero, zero), unroll=UNROLL)
    lane = lax.broadcasted_iota(jnp.int32, (PACKED, LANES), 1)
    image = jnp.zeros((PACKED, LANES), f32)
    for w in range(WINDOWS):
        cosine, sine = tables(w, slice(0, PATCHES))
        column = jnp.sum(cosine * q_re - sine * q_im, axis=1, keepdims=True)
        for q in range(4):
            image = jnp.where(lane == q * WINDOWS + w, column[q * PACKED : (q + 1) * PACKED], image)
    used = lax.broadcasted_iota(jnp.int32, (16, 8, LANES), 1) < PARTS
    u = jnp.where(used, u_ref[...], 0.0)
    ss = jnp.sum(jnp.sum(u * u, axis=0), axis=0, keepdims=True)
    for d in range(16):
        buf_ref[d, :PACKED, :] = image
        buf_ref[d, PACKED:, :] = jnp.broadcast_to(ss, (IMAGE - PACKED, LANES))


def first_adjoint(green_ref, cos_a, sin_a, onset_ref, buf_ref, u_ref, cos_b, sin_b):
    fill_tables(onset_ref, range(3, 4), cos_b, sin_b)
    for s in range(16):
        terms = [green_ref[s, GREEN_ROWS + 8 * t : GREEN_ROWS + 8 * t + 8, :].astype(f32) for t in range(TERMS)]
        u_ref[s] = sum(terms)
    data_to_model(u_ref, green_ref, tables_of((cos_a, sin_a, cos_b, sin_b)), buf_ref)


def norm_of(row):
    return jnp.broadcast_to(jnp.sqrt(jnp.sum(row, axis=1, keepdims=True)), (1, LANES))


def next_adjoint(green_ref, t0, t1, t2, t3, d0, d1, d2, d3, left_ref, right_ref, buf_ref, u_ref):
    data = (d0[...] + d1[...]) + (d2[...] + d3[...])
    alpha = norm_of(data[0, SQUARES : SQUARES + 1])
    beta = right_ref[PACKED : PACKED + 1]
    u_ref[...] = data / alpha[None] - alpha[None] * (left_ref[...] / beta[None])
    u_ref[0, SQUARES : SQUARES + 1, :] = alpha
    data_to_model(u_ref, green_ref, tables_of((t0, t1, t2, t3)), buf_ref)


def new_right(image_ref, right_ref, prev_ref, left_ref):
    image = jnp.sum(image_ref[...], axis=0)
    beta = norm_of(image[PACKED : PACKED + 1])
    right = image[:PACKED] / beta
    if prev_ref is not None:
        right = right - beta * (prev_ref[:PACKED] / left_ref[0, SQUARES : SQUARES + 1])
    right_ref[:PACKED] = right
    right_ref[PACKED:] = jnp.broadcast_to(beta, (IMAGE - PACKED, LANES))
    return right, jnp.sum(right * right, axis=0, keepdims=True)


def forward(first, green_ref, t0, t1, t2, t3, image_ref, *refs):
    prev_ref, left_ref, data_ref, right_ref, spec = ((None, None) + refs) if first else refs
    right, ss = new_right(image_ref, right_ref, prev_ref, left_ref)
    model_to_data(right, ss, green_ref, tables_of((t0, t1, t2, t3)), data_ref, spec)


def last_right(image_ref, prev_ref, left_ref, right_ref, ss_ref, give_ref):
    right, ss = new_right(image_ref, right_ref, prev_ref, left_ref)
    ss_ref[...] = jnp.broadcast_to(ss, (8, LANES))
    give_ref[...] = left_ref[lax.axis_index(STA) ^ 2]


def finish(s0, s1, s2, s3, v0_ref, v1_ref, v2_ref, u1_ref, u2_ref, half_ref, slip_ref, direction_ref, misfit_ref, scale):
    zl, win = lax.axis_index(ZL), lax.axis_index(WIN)
    squares = (s0[...] + s1[...]) + (s2[...] + s3[...])
    at = slice(PACKED, PACKED + 1)
    alphas = [u1_ref[0, SQUARES : SQUARES + 1], u2_ref[0, SQUARES : SQUARES + 1], norm_of(squares[0:1])]
    betas = [v0_ref[at], v1_ref[at], v2_ref[at]]
    rights = [ref[:PACKED] / a for ref, a in zip((v0_ref, v1_ref, v2_ref), alphas)]
    phi_bar, rho_bar = betas[0], alphas[0]
    search, estimate = rights[0], jnp.zeros((PACKED, LANES), f32)
    for alpha, beta, right in zip(alphas[1:], betas[1:], rights[1:]):
        rho = jnp.sqrt(rho_bar * rho_bar + beta * beta)
        cosine, sine = rho_bar / rho, beta / rho
        theta = sine * alpha
        rho_bar = -cosine * alpha
        phi = cosine * phi_bar
        phi_bar = sine * phi_bar
        estimate = estimate + phi / rho * search
        search = right - theta / rho * search
    for value, ref in ((estimate, slip_ref), (search * scale, direction_ref)):
        for h in range(2):
            left = (2 * zl + h) * WINDOWS + win * 4
            rolled = pltpu.roll(value, LANES - left, 1)
            ref[:, h * PACKED : (h + 1) * PACKED] = jnp.transpose(rolled, (1, 0))[:4]
    own = u2_ref[lax.axis_index(STA)]
    other = half_ref[...]
    for comp in range(COMP):
        rows = slice(2 * comp, 2 * comp + 2)
        for h in range(2):
            value = jnp.where(zl == h, own[rows], other[rows])
            misfit_ref[0, comp, :, h * LANES : (h + 1) * LANES] = value / betas[2] * phi_bar


def from_partners(array, axis, at=range(4)):
    held = {k: lax.ppermute(array, axis, [(at[i], at[i ^ k]) for i in range(4)]) for k in ORDER}
    return [held[k] for k in (1, 2, 3)]


def other_core(array):
    return lax.ppermute(array, C, [(0, 1), (1, 0)])


def summed_over_patches(array):
    both = array + other_core(array)
    side = lax.ppermute(both, (X, C), [(x * 2 + c, (x ^ (1, 3)[c]) * 2 + c) for x in range(4) for c in range(2)])
    across = lax.ppermute(both, X, [(x, x ^ 2) for x in range(4)])
    return [both, across, side, other_core(side)]


def summed_over_frequencies(buf):
    return lax.all_to_all(buf, (ZL, Y, ZH), 0, 0, tiled=True)


def local(green, records, onsets, mask):
    packed = pack(mask, green, records).reshape(16, ROWS, LANES)
    packed, onset_rows = lax.optimization_barrier((packed, onsets.T[None]))
    arrived = lax.all_to_all(packed, STA, 0, 0, tiled=True)
    rows = jnp.concatenate([onset_rows, *from_partners(onset_rows, Y)], axis=0)
    gathered = jnp.stack([rows, *from_partners(rows, (ZL, ZH), (0, 2, 1, 3))])
    head, tail = ((SPLIT, PATCHES, LANES), f32), ((WINDOWS - SPLIT, PATCHES, LANES), f32)
    tables = call(table_body, [head, head], gathered)

    buf_shape, data_shape, right_shape = ((16, IMAGE, LANES), f32), ((16, 8, LANES), f32), ((IMAGE, LANES), f32)

    def forward_call(first, *args):
        return pl.pallas_call(
            functools.partial(forward, first),
            in_specs=[VMEM] * len(args),
            out_specs=[VMEM] * 2,
            out_shape=[jax.ShapeDtypeStruct(*data_shape), jax.ShapeDtypeStruct(*right_shape)],
            scratch_shapes=[pltpu.VMEM((2, PATCHES, LANES), f32)],
            compiler_params=PARAMS,
            cost_estimate=pl.CostEstimate(flops=2_000_000, bytes_accessed=4_000_000, transcendentals=0),
        )(*args)

    buf, u0, *rest = call(first_adjoint, [buf_shape, data_shape, tail, tail], arrived, *tables, gathered)
    base = (arrived, *tables, *rest)
    data, v0 = forward_call(True, *base, summed_over_frequencies(buf))
    buf, u1 = call(next_adjoint, [buf_shape, data_shape], *base, *summed_over_patches(data), u0, v0)
    data, v1 = forward_call(False, *base, summed_over_frequencies(buf), v0, u1)
    buf, u2 = call(next_adjoint, [buf_shape, data_shape], *base, *summed_over_patches(data), u1, v1)
    tile = ((8, LANES), f32)
    v2, ss, give = call(last_right, [right_shape, tile, tile], summed_over_frequencies(buf), v1, u2)
    half = lax.ppermute(give, ZL, [(0, 1), (1, 0)])
    scale = math.sqrt(512 * 32)
    slip, direction, misfit = call(
        functools.partial(finish, scale=scale),
        [((4, 32), f32), ((4, 32), f32), ((1, COMP, 2, 256), f32)],
        *summed_over_patches(ss), v0, v1, v2, u1, u2, half,
    )
    return slip.T, direction.T, misfit


def solution(mesh):
    finer = Mesh(mesh.devices.reshape(4, 2, 2, 4, 2), (X, ZL, C, Y, ZH))
    return jax.shard_map(
        local,
        mesh=finer,
        in_specs=(P(STA, None, None, None, WIN), P(STA, None, None, WIN), P(STA, WIN), P(STA, None)),
        out_specs=(P(STA, WIN), P(STA, WIN), P(STA, None, None, WIN)),
        check_vma=False,
    )
```

```python
import functools
import math

import jax
import jax.numpy as jnp
from jax import lax
from jax.experimental import pallas as pl
from jax.experimental.pallas import tpu as pltpu
from jax.sharding import Mesh
from jax.sharding import PartitionSpec as P

X, ZL, C, Y, ZH = "x", "zl", "core", "y", "zh"
STA = (X, ZL, C)
WIN = (Y, ZH)
SAMPLES = 4096
LANES = 128
COMP = 3
PARTS = 2 * COMP
PATCHES = 64
GREEN_ROWS = PARTS * PATCHES
TERMS = 2
ROWS = GREEN_ROWS + 8 * TERMS
PACKED = 16
IMAGE = 24
SQUARES = 6
f32, bf16 = jnp.float32, jnp.bfloat16
VMEM = pl.BlockSpec(memory_space=pltpu.VMEM)
HBM = pl.BlockSpec(memory_space=pltpu.HBM)
UNROLL = 4
ORDER = (3, 1, 2)
SPLIT = 14
PARAMS = pltpu.CompilerParams(vmem_limit_bytes=16 << 20)


def call(body, outs, *args, scratch=()):
    return pl.pallas_call(
        body,
        in_specs=[VMEM] * len(args),
        out_specs=[VMEM] * len(outs),
        out_shape=[jax.ShapeDtypeStruct(s, d) for s, d in outs],
        scratch_shapes=list(scratch),
        compiler_params=PARAMS,
        cost_estimate=pl.CostEstimate(flops=2_000_000, bytes_accessed=4_000_000, transcendentals=0),
    )(*args)


def pack_body(mask_hbm, green_hbm, rec_hbm, out_hbm, mask_ref, green_ref, rec_ref, out_ref, rows, in_sems, out_sems):
    reads = [pltpu.make_async_copy(green_hbm.at[0, k // 2, k % 2], green_ref.at[k], in_sems.at[k]) for k in range(PARTS)]
    reads.append(pltpu.make_async_copy(rec_hbm.at[0], rec_ref, in_sems.at[PARTS]))
    reads.append(pltpu.make_async_copy(mask_hbm, mask_ref, in_sems.at[PARTS + 1]))
    for read in reversed(reads):
        read.start()
    reads[PARTS + 1].wait()
    reads[PARTS].wait()
    rows[...] = jnp.zeros_like(rows)
    for comp in range(COMP):
        rows[2 * comp : 2 * comp + 2, :] = jnp.where(mask_ref[0, comp] != 0, rec_ref[comp], 0.0)
    for half in range(2):
        rest = rows[:, half * LANES : (half + 1) * LANES]
        for term in range(TERMS):
            piece = rest.astype(bf16)
            rest = rest - piece.astype(f32)
            at = GREEN_ROWS + 8 * term
            for x in range(4):
                for c in range(2):
                    out_ref[x, half, c, at : at + 8, :] = piece
    writes = []
    for k in range(PARTS + 1):
        if k < PARTS:
            used = mask_ref[0, k // 2] != 0
            reads[k].wait()
            for x in range(4):
                for zl in range(2):
                    for c in range(2):
                        at = x * 128 + zl * 64 + c * 32
                        block = green_ref[k, at : at + 32, :]
                        block = jnp.where(used, block, jnp.zeros_like(block))
                        to = k * PATCHES + zl * 32
                        for half in range(2):
                            out_ref[x, half, c, to : to + 32, :] = block[:, half * LANES : (half + 1) * LANES]
        span = pl.ds(k * PATCHES, PATCHES if k < PARTS else 8 * TERMS)
        write = pltpu.make_async_copy(out_ref.at[:, :, :, span], out_hbm.at[:, :, :, span], out_sems.at[k])
        write.start()
        writes.append(write)
    for write in writes:
        write.wait()


def pack(mask, green, records):
    held = (4, 2, 2, ROWS, LANES)
    return pl.pallas_call(
        pack_body,
        in_specs=[HBM] * 3,
        out_specs=HBM,
        out_shape=jax.ShapeDtypeStruct(held, bf16),
        scratch_shapes=[
            pltpu.SMEM((1, COMP), jnp.int32),
            pltpu.VMEM((PARTS, 512, 256), bf16),
            pltpu.VMEM((COMP, 2, 256), f32),
            pltpu.VMEM(held, bf16),
            pltpu.VMEM((8, 256), f32),
            pltpu.SemaphoreType.DMA((PARTS + 2,)),
            pltpu.SemaphoreType.DMA((PARTS + 1,)),
        ],
        cost_estimate=pl.CostEstimate(flops=4_000_000, bytes_accessed=4_000_000, transcendentals=0),
    )(mask, green, records)


def fill_tables(onset_ref, first_pair, last_pair, cos_ref, sin_ref):
    y, z = lax.axis_index(Y), lax.axis_index(ZH) * 2 + lax.axis_index(ZL)
    first = lax.axis_index(WIN) * 256 + lax.axis_index(ZL) * LANES
    freq = lax.broadcasted_iota(jnp.int32, (LANES, LANES), 0) + first
    for pair in range(first_pair, last_pair):
        block, a = pair // 2, pair % 2
        pieces = [onset_ref[z ^ (block % 2 * 2 + zl), y ^ (block // 2)] for zl in range(2)]
        onset = jnp.concatenate([pieces[zl][2 * a + one : 2 * a + one + 1] for one in range(2) for zl in range(2)], axis=1)
        turns = onset * freq + SAMPLES // 8
        quarter = lax.shift_right_logical(turns, 10) & 3
        angle = ((turns & (SAMPLES // 4 - 1)) - SAMPLES // 8).astype(f32) * (2.0 * math.pi / SAMPLES)
        t = angle * angle
        s = angle * (1.0 + t * (-1 / 6 + t * (1 / 120 + t * (-1 / 5040 + t * (1 / 362880)))))
        c = 1.0 + t * (-0.5 + t * (1 / 24 + t * (-1 / 720 + t * (1 / 40320 + t * (-1 / 3628800)))))
        odd = (quarter & 1) == 1
        cosine = jnp.where(odd, s, c)
        sine = jnp.where(odd, c, s)
        cos_ref[pair - first_pair] = jnp.where((quarter == 1) | (quarter == 2), -cosine, cosine)
        sin_ref[pair - first_pair] = jnp.where(quarter >= 2, -sine, sine)


def table_body(onset_ref, cos_ref, sin_ref):
    fill_tables(onset_ref, 0, SPLIT, cos_ref, sin_ref)


def tables_of(refs):
    cos_a, sin_a, cos_b, sin_b = refs
    return lambda pair: (cos_a[pair], sin_a[pair]) if pair < SPLIT else (cos_b[pair - SPLIT], sin_b[pair - SPLIT])


def model_to_data(model_ref, ss, green_ref, tables, data_ref):
    re = jnp.zeros((LANES, LANES), f32)
    im = jnp.zeros((LANES, LANES), f32)
    for pair in range(PACKED):
        cosine, sine = tables(pair)
        v = model_ref[pair : pair + 1, :]
        re = re + v * cosine
        im = im - v * sine
    re, im = jnp.transpose(re, (1, 0)), jnp.transpose(im, (1, 0))
    re, im = re[:PATCHES] + re[PATCHES:], im[:PATCHES] + im[PATCHES:]
    zero = jnp.zeros((2, LANES), f32)

    def station(s, carry):
        for comp in range(COMP):
            at = 2 * comp * PATCHES
            g_re = green_ref[s, at : at + PATCHES, :].astype(f32)
            g_im = green_ref[s, at + PATCHES : at + 2 * PATCHES, :].astype(f32)
            data_ref[s, 2 * comp : 2 * comp + 1, :] = jnp.sum(g_re * re - g_im * im, axis=0, keepdims=True)
            data_ref[s, 2 * comp + 1 : 2 * comp + 2, :] = jnp.sum(g_re * im + g_im * re, axis=0, keepdims=True)
        data_ref[s, SQUARES:, :] = zero
        return carry

    lax.fori_loop(0, 16, station, 0, unroll=UNROLL)
    data_ref[0, SQUARES : SQUARES + 1, :] = ss


def data_to_model(u_ref, green_ref, tables, buf_ref):
    def station(s, carry):
        q_re, q_im = carry
        for comp in range(COMP):
            at = 2 * comp * PATCHES
            g_re = green_ref[s, at : at + PATCHES, :].astype(f32)
            g_im = green_ref[s, at + PATCHES : at + 2 * PATCHES, :].astype(f32)
            u_re = u_ref[s, 2 * comp : 2 * comp + 1, :]
            u_im = u_ref[s, 2 * comp + 1 : 2 * comp + 2, :]
            q_re = q_re + (g_re * u_re + g_im * u_im)
            q_im = q_im + (g_re * u_im - g_im * u_re)
        return q_re, q_im

    zero = jnp.zeros((PATCHES, LANES), f32)
    q_re, q_im = lax.fori_loop(0, 16, station, (zero, zero), unroll=UNROLL)
    q_re, q_im = (jnp.transpose(jnp.concatenate([q, q], axis=0), (1, 0)) for q in (q_re, q_im))
    for pair in range(PACKED):
        cosine, sine = tables(pair)
        buf_ref[0, pair : pair + 1, :] = jnp.sum(cosine * q_re - sine * q_im, axis=0, keepdims=True)
    used = lax.broadcasted_iota(jnp.int32, (16, 8, LANES), 1) < PARTS
    u = jnp.where(used, u_ref[...], 0.0)
    ss = jnp.sum(jnp.sum(u * u, axis=0), axis=0, keepdims=True)
    buf_ref[0, PACKED:, :] = jnp.broadcast_to(ss, (IMAGE - PACKED, LANES))
    image = buf_ref[0]
    for d in range(1, 16):
        buf_ref[d] = image


def first_adjoint(green_ref, cos_a, sin_a, onset_ref, buf_ref, u_ref, cos_b, sin_b):
    fill_tables(onset_ref, SPLIT, PACKED, cos_b, sin_b)
    for s in range(16):
        terms = [green_ref[s, GREEN_ROWS + 8 * t : GREEN_ROWS + 8 * t + 8, :].astype(f32) for t in range(TERMS)]
        u_ref[s] = sum(terms)
    data_to_model(u_ref, green_ref, tables_of((cos_a, sin_a, cos_b, sin_b)), buf_ref)


def norm_of(row):
    return jnp.broadcast_to(jnp.sqrt(jnp.sum(row, axis=1, keepdims=True)), (1, LANES))


def next_adjoint(green_ref, t0, t1, t2, t3, d0, d1, d2, d3, left_ref, right_ref, buf_ref, u_ref):
    data = (d0[...] + d1[...]) + (d2[...] + d3[...])
    alpha = norm_of(data[0, SQUARES : SQUARES + 1])
    beta = right_ref[PACKED : PACKED + 1]
    u_ref[...] = data / alpha[None] - alpha[None] * (left_ref[...] / beta[None])
    u_ref[0, SQUARES : SQUARES + 1, :] = alpha
    data_to_model(u_ref, green_ref, tables_of((t0, t1, t2, t3)), buf_ref)


def new_right(image_ref, right_ref, prev_ref, left_ref):
    image = jnp.sum(image_ref[...], axis=0)
    beta = norm_of(image[PACKED : PACKED + 1])
    right = image[:PACKED] / beta
    if prev_ref is not None:
        right = right - beta * (prev_ref[:PACKED] / left_ref[0, SQUARES : SQUARES + 1])
    right_ref[:PACKED] = right
    right_ref[PACKED:] = jnp.broadcast_to(beta, (IMAGE - PACKED, LANES))
    return jnp.sum(right * right, axis=0, keepdims=True)


def forward(first, green_ref, t0, t1, t2, t3, image_ref, *refs):
    prev_ref, left_ref, data_ref, right_ref = ((None, None) + refs) if first else refs
    ss = new_right(image_ref, right_ref, prev_ref, left_ref)
    model_to_data(right_ref, ss, green_ref, tables_of((t0, t1, t2, t3)), data_ref)


def last_right(image_ref, prev_ref, left_ref, right_ref, ss_ref, give_ref):
    ss = new_right(image_ref, right_ref, prev_ref, left_ref)
    ss_ref[...] = jnp.broadcast_to(ss, (8, LANES))
    give_ref[...] = left_ref[lax.axis_index(STA) ^ 2]


def finish(s0, s1, s2, s3, v0_ref, v1_ref, v2_ref, u1_ref, u2_ref, half_ref, slip_ref, direction_ref, misfit_ref, rows_ref, scale):
    zl, win = lax.axis_index(ZL), lax.axis_index(WIN)
    squares = (s0[...] + s1[...]) + (s2[...] + s3[...])
    at = slice(PACKED, PACKED + 1)
    alphas = [u1_ref[0, SQUARES : SQUARES + 1], u2_ref[0, SQUARES : SQUARES + 1], norm_of(squares[0:1])]
    betas = [v0_ref[at], v1_ref[at], v2_ref[at]]
    rights = [ref[:PACKED] / a for ref, a in zip((v0_ref, v1_ref, v2_ref), alphas)]
    phi_bar, rho_bar = betas[0], alphas[0]
    search, estimate = rights[0], jnp.zeros((PACKED, LANES), f32)
    for alpha, beta, right in zip(alphas[1:], betas[1:], rights[1:]):
        rho = jnp.sqrt(rho_bar * rho_bar + beta * beta)
        cosine, sine = rho_bar / rho, beta / rho
        theta = sine * alpha
        rho_bar = -cosine * alpha
        phi = cosine * phi_bar
        phi_bar = sine * phi_bar
        estimate = estimate + phi / rho * search
        search = right - theta / rho * search
    for value, ref in ((estimate, slip_ref), (search * scale, direction_ref)):
        rows_ref[...] = pltpu.roll(value, LANES - zl * 32, 1)
        for a in range(2):
            row = rows_ref[pl.ds(win * 2 + a, 1), :]
            for one in range(2):
                ref[2 * a + one : 2 * a + one + 1, :] = row[:, one * 64 : one * 64 + 32]
    own = u2_ref[lax.axis_index(STA)]
    other = half_ref[...]
    for comp in range(COMP):
        rows = slice(2 * comp, 2 * comp + 2)
        for h in range(2):
            value = jnp.where(zl == h, own[rows], other[rows])
            misfit_ref[0, comp, :, h * LANES : (h + 1) * LANES] = value / betas[2] * phi_bar


def from_partners(array, axis, at=range(4)):
    held = {k: lax.ppermute(array, axis, [(at[i], at[i ^ k]) for i in range(4)]) for k in ORDER}
    return [held[k] for k in (1, 2, 3)]


def other_core(array):
    return lax.ppermute(array, C, [(0, 1), (1, 0)])


def summed_over_patches(array):
    both = array + other_core(array)
    side = lax.ppermute(both, (X, C), [(x * 2 + c, (x ^ (1, 3)[c]) * 2 + c) for x in range(4) for c in range(2)])
    across = lax.ppermute(both, X, [(x, x ^ 2) for x in range(4)])
    return [both, across, side, other_core(side)]


def summed_over_frequencies(buf):
    return lax.all_to_all(buf, (ZL, Y, ZH), 0, 0, tiled=True)


def local(green, records, onsets, mask):
    packed = pack(mask, green, records).reshape(16, ROWS, LANES)
    packed, onset_rows = lax.optimization_barrier((packed, onsets.T[None]))
    arrived = lax.all_to_all(packed, STA, 0, 0, tiled=True)
    rows = jnp.concatenate([onset_rows, *from_partners(onset_rows, Y)], axis=0)
    gathered = jnp.stack([rows, *from_partners(rows, (ZL, ZH), (0, 2, 1, 3))])
    head, tail = ((SPLIT, LANES, LANES), f32), ((PACKED - SPLIT, LANES, LANES), f32)
    tables = call(table_body, [head, head], gathered)

    buf_shape, data_shape, right_shape = ((16, IMAGE, LANES), f32), ((16, 8, LANES), f32), ((IMAGE, LANES), f32)

    def forward_call(first, *args):
        return pl.pallas_call(
            functools.partial(forward, first),
            in_specs=[VMEM] * len(args),
            out_specs=[VMEM] * 2,
            out_shape=[jax.ShapeDtypeStruct(*data_shape), jax.ShapeDtypeStruct(*right_shape)],
            compiler_params=PARAMS,
            cost_estimate=pl.CostEstimate(flops=2_000_000, bytes_accessed=4_000_000, transcendentals=0),
        )(*args)

    buf, u0, *rest = call(first_adjoint, [buf_shape, data_shape, tail, tail], arrived, *tables, gathered)
    base = (arrived, *tables, *rest)
    data, v0 = forward_call(True, *base, summed_over_frequencies(buf))
    buf, u1 = call(next_adjoint, [buf_shape, data_shape], *base, *summed_over_patches(data), u0, v0)
    data, v1 = forward_call(False, *base, summed_over_frequencies(buf), v0, u1)
    buf, u2 = call(next_adjoint, [buf_shape, data_shape], *base, *summed_over_patches(data), u1, v1)
    tile = ((8, LANES), f32)
    v2, ss, give = call(last_right, [right_shape, tile, tile], summed_over_frequencies(buf), v1, u2)
    half = lax.ppermute(give, ZL, [(0, 1), (1, 0)])
    scale = math.sqrt(512 * 32)
    slip, direction, misfit = call(
        functools.partial(finish, scale=scale),
        [((4, 32), f32), ((4, 32), f32), ((1, COMP, 2, 256), f32)],
        *summed_over_patches(ss), v0, v1, v2, u1, u2, half,
        scratch=[pltpu.VMEM((PACKED, LANES), f32)],
    )
    return slip.T, direction.T, misfit


def solution(mesh):
    finer = Mesh(mesh.devices.reshape(4, 2, 2, 4, 2), (X, ZL, C, Y, ZH))
    return jax.shard_map(
        local,
        mesh=finer,
        in_specs=(P(STA, None, None, None, WIN), P(STA, None, None, WIN), P(STA, WIN), P(STA, None)),
        out_specs=(P(STA, WIN), P(STA, WIN), P(STA, None, None, WIN)),
        check_vma=False,
    )
```

```python
import functools
import math

import jax
import jax.numpy as jnp
from jax import lax
from jax.experimental import pallas as pl
from jax.experimental.pallas import tpu as pltpu
from jax.sharding import Mesh
from jax.sharding import PartitionSpec as P

X, ZL, C, Y, ZH = "x", "zl", "core", "y", "zh"
STA = (X, ZL, C)
WIN = (Y, ZH)
SAMPLES = 4096
LANES = 128
COMP = 3
PARTS = 2 * COMP
PATCHES = 64
GREEN_ROWS = PARTS * PATCHES
TERMS = 2
ROWS = GREEN_ROWS + 8 * TERMS
PACKED = 16
IMAGE = 24
HALF = PACKED + 1
SQUARES = 6
f32, bf16 = jnp.float32, jnp.bfloat16
VMEM = pl.BlockSpec(memory_space=pltpu.VMEM)
HBM = pl.BlockSpec(memory_space=pltpu.HBM)
UNROLL = 4
ORDER = (3, 1, 2)
SPLIT = 14
PARAMS = pltpu.CompilerParams(vmem_limit_bytes=16 << 20)


def call(body, outs, *args, scratch=()):
    return pl.pallas_call(
        body,
        in_specs=[VMEM] * len(args),
        out_specs=[VMEM] * len(outs),
        out_shape=[jax.ShapeDtypeStruct(s, d) for s, d in outs],
        scratch_shapes=list(scratch),
        compiler_params=PARAMS,
        cost_estimate=pl.CostEstimate(flops=2_000_000, bytes_accessed=4_000_000, transcendentals=0),
    )(*args)


def pack_body(mask_hbm, green_hbm, rec_hbm, out_hbm, mask_ref, green_ref, rec_ref, out_ref, rows, in_sems, out_sems):
    reads = [pltpu.make_async_copy(green_hbm.at[0, k // 2, k % 2], green_ref.at[k], in_sems.at[k]) for k in range(PARTS)]
    reads.append(pltpu.make_async_copy(rec_hbm.at[0], rec_ref, in_sems.at[PARTS]))
    reads.append(pltpu.make_async_copy(mask_hbm, mask_ref, in_sems.at[PARTS + 1]))
    for read in reversed(reads):
        read.start()
    reads[PARTS + 1].wait()
    reads[PARTS].wait()
    rows[...] = jnp.zeros_like(rows)
    for comp in range(COMP):
        rows[2 * comp : 2 * comp + 2, :] = jnp.where(mask_ref[0, comp] != 0, rec_ref[comp], 0.0)
    for half in range(2):
        rest = rows[:, half * LANES : (half + 1) * LANES]
        for term in range(TERMS):
            piece = rest.astype(bf16)
            rest = rest - piece.astype(f32)
            at = GREEN_ROWS + 8 * term
            for x in range(4):
                for c in range(2):
                    out_ref[x, half, c, at : at + 8, :] = piece
    writes = []
    for k in range(PARTS + 1):
        if k < PARTS:
            used = mask_ref[0, k // 2] != 0
            reads[k].wait()
            for x in range(4):
                for zl in range(2):
                    for c in range(2):
                        at = x * 128 + zl * 64 + c * 32
                        block = green_ref[k, at : at + 32, :]
                        block = jnp.where(used, block, jnp.zeros_like(block))
                        to = k * PATCHES + zl * 32
                        for half in range(2):
                            out_ref[x, half, c, to : to + 32, :] = block[:, half * LANES : (half + 1) * LANES]
        span = pl.ds(k * PATCHES, PATCHES if k < PARTS else 8 * TERMS)
        write = pltpu.make_async_copy(out_ref.at[:, :, :, span], out_hbm.at[:, :, :, span], out_sems.at[k])
        write.start()
        writes.append(write)
    for write in writes:
        write.wait()


def pack(mask, green, records):
    held = (4, 2, 2, ROWS, LANES)
    return pl.pallas_call(
        pack_body,
        in_specs=[HBM] * 3,
        out_specs=HBM,
        out_shape=jax.ShapeDtypeStruct(held, bf16),
        scratch_shapes=[
            pltpu.SMEM((1, COMP), jnp.int32),
            pltpu.VMEM((PARTS, 512, 256), bf16),
            pltpu.VMEM((COMP, 2, 256), f32),
            pltpu.VMEM(held, bf16),
            pltpu.VMEM((8, 256), f32),
            pltpu.SemaphoreType.DMA((PARTS + 2,)),
            pltpu.SemaphoreType.DMA((PARTS + 1,)),
        ],
        cost_estimate=pl.CostEstimate(flops=4_000_000, bytes_accessed=4_000_000, transcendentals=0),
    )(mask, green, records)


def fill_tables(onset_ref, first_pair, last_pair, cos_ref, sin_ref):
    y, z = lax.axis_index(Y), lax.axis_index(ZH) * 2 + lax.axis_index(ZL)
    first = lax.axis_index(WIN) * 256 + lax.axis_index(ZL) * LANES
    freq = lax.broadcasted_iota(jnp.int32, (LANES, LANES), 0) + first
    for pair in range(first_pair, last_pair):
        block, a = pair // 2, pair % 2
        pieces = [onset_ref[z ^ (block % 2 * 2 + zl), y ^ (block // 2)] for zl in range(2)]
        onset = jnp.concatenate([pieces[zl][2 * a + one : 2 * a + one + 1] for one in range(2) for zl in range(2)], axis=1)
        turns = onset * freq + SAMPLES // 8
        quarter = lax.shift_right_logical(turns, 10) & 3
        angle = ((turns & (SAMPLES // 4 - 1)) - SAMPLES // 8).astype(f32) * (2.0 * math.pi / SAMPLES)
        t = angle * angle
        s = angle * (1.0 + t * (-1 / 6 + t * (1 / 120 + t * (-1 / 5040 + t * (1 / 362880)))))
        c = 1.0 + t * (-0.5 + t * (1 / 24 + t * (-1 / 720 + t * (1 / 40320 + t * (-1 / 3628800)))))
        odd = (quarter & 1) == 1
        cosine = jnp.where(odd, s, c)
        sine = jnp.where(odd, c, s)
        cos_ref[pair - first_pair] = jnp.where((quarter == 1) | (quarter == 2), -cosine, cosine)
        sin_ref[pair - first_pair] = jnp.where(quarter >= 2, -sine, sine)


def table_body(onset_ref, cos_ref, sin_ref):
    fill_tables(onset_ref, 0, SPLIT, cos_ref, sin_ref)


def tables_of(refs):
    cos_a, sin_a, cos_b, sin_b = refs
    return lambda pair: (cos_a[pair], sin_a[pair]) if pair < SPLIT else (cos_b[pair - SPLIT], sin_b[pair - SPLIT])


def model_to_data(model_ref, ss, green_ref, tables, data_ref):
    re = jnp.zeros((LANES, LANES), f32)
    im = jnp.zeros((LANES, LANES), f32)
    for pair in range(PACKED):
        cosine, sine = tables(pair)
        v = model_ref[pair : pair + 1, :]
        re = re + v * cosine
        im = im - v * sine
    re, im = jnp.transpose(re, (1, 0)), jnp.transpose(im, (1, 0))
    re, im = re[:PATCHES] + re[PATCHES:], im[:PATCHES] + im[PATCHES:]
    zero = jnp.zeros((2, LANES), f32)

    def station(s, carry):
        for comp in range(COMP):
            at = 2 * comp * PATCHES
            g_re = green_ref[s, at : at + PATCHES, :].astype(f32)
            g_im = green_ref[s, at + PATCHES : at + 2 * PATCHES, :].astype(f32)
            data_ref[s, 2 * comp : 2 * comp + 1, :] = jnp.sum(g_re * re - g_im * im, axis=0, keepdims=True)
            data_ref[s, 2 * comp + 1 : 2 * comp + 2, :] = jnp.sum(g_re * im + g_im * re, axis=0, keepdims=True)
        data_ref[s, SQUARES:, :] = zero
        return carry

    lax.fori_loop(0, 16, station, 0, unroll=UNROLL)
    data_ref[0, SQUARES : SQUARES + 1, :] = ss


def data_to_model(u_ref, green_ref, tables, buf_ref):
    def station(s, carry):
        q_re, q_im = carry
        for comp in range(COMP):
            at = 2 * comp * PATCHES
            g_re = green_ref[s, at : at + PATCHES, :].astype(f32)
            g_im = green_ref[s, at + PATCHES : at + 2 * PATCHES, :].astype(f32)
            u_re = u_ref[s, 2 * comp : 2 * comp + 1, :]
            u_im = u_ref[s, 2 * comp + 1 : 2 * comp + 2, :]
            q_re = q_re + (g_re * u_re + g_im * u_im)
            q_im = q_im + (g_re * u_im - g_im * u_re)
        return q_re, q_im

    zero = jnp.zeros((PATCHES, LANES), f32)
    q_re, q_im = lax.fori_loop(0, 16, station, (zero, zero), unroll=UNROLL)
    q_re, q_im = (jnp.transpose(jnp.concatenate([q, q], axis=0), (1, 0)) for q in (q_re, q_im))
    for pair in range(PACKED):
        cosine, sine = tables(pair)
        buf_ref[0, pair : pair + 1, :] = jnp.sum(cosine * q_re - sine * q_im, axis=0, keepdims=True)
    used = lax.broadcasted_iota(jnp.int32, (16, 8, LANES), 1) < PARTS
    u = jnp.where(used, u_ref[...], 0.0)
    ss = jnp.sum(jnp.sum(u * u, axis=0), axis=0, keepdims=True)
    buf_ref[0, PACKED:, :] = jnp.broadcast_to(ss, (IMAGE - PACKED, LANES))
    buf_ref[0, HALF : HALF + PARTS, :] = u_ref[lax.axis_index(STA) ^ 2, :PARTS, :]
    image = buf_ref[0]
    for d in range(1, 16):
        buf_ref[d] = image


def first_adjoint(green_ref, cos_a, sin_a, onset_ref, buf_ref, u_ref, cos_b, sin_b):
    fill_tables(onset_ref, SPLIT, PACKED, cos_b, sin_b)
    for s in range(16):
        terms = [green_ref[s, GREEN_ROWS + 8 * t : GREEN_ROWS + 8 * t + 8, :].astype(f32) for t in range(TERMS)]
        u_ref[s] = sum(terms)
    data_to_model(u_ref, green_ref, tables_of((cos_a, sin_a, cos_b, sin_b)), buf_ref)


def norm_of(row):
    return jnp.broadcast_to(jnp.sqrt(jnp.sum(row, axis=1, keepdims=True)), (1, LANES))


def next_adjoint(green_ref, t0, t1, t2, t3, d0, d1, d2, d3, left_ref, right_ref, buf_ref, u_ref):
    data = (d0[...] + d1[...].astype(f32)) + (d2[...].astype(f32) + d3[...].astype(f32))
    alpha = norm_of(data[0, SQUARES : SQUARES + 1] + data[0, SQUARES + 1 :])
    beta = right_ref[PACKED : PACKED + 1]
    u_ref[...] = data / alpha[None] - alpha[None] * (left_ref[...] / beta[None])
    u_ref[0, SQUARES : SQUARES + 1, :] = alpha
    data_to_model(u_ref, green_ref, tables_of((t0, t1, t2, t3)), buf_ref)


def new_right(image_ref, right_ref, prev_ref, left_ref):
    image = jnp.sum(image_ref[...], axis=0)
    beta = norm_of(image[PACKED : PACKED + 1])
    right = image[:PACKED] / beta
    if prev_ref is not None:
        right = right - beta * (prev_ref[:PACKED] / left_ref[0, SQUARES : SQUARES + 1])
    right_ref[:PACKED] = right
    right_ref[PACKED:] = jnp.broadcast_to(beta, (IMAGE - PACKED, LANES))
    return jnp.sum(right * right, axis=0, keepdims=True)


def forward(first, green_ref, t0, t1, t2, t3, image_ref, *refs):
    prev_ref, left_ref, data_ref, right_ref = ((None, None) + refs) if first else refs
    ss = new_right(image_ref, right_ref, prev_ref, left_ref)
    model_to_data(right_ref, ss, green_ref, tables_of((t0, t1, t2, t3)), data_ref)


def last_right(image_ref, prev_ref, left_ref, right_ref, ss_ref):
    ss = new_right(image_ref, right_ref, prev_ref, left_ref)
    ss_ref[...] = jnp.broadcast_to(ss, (8, LANES))


def finish(s0, s1, s2, s3, v0_ref, v1_ref, v2_ref, u1_ref, u2_ref, image_ref, slip_ref, direction_ref, misfit_ref, rows_ref, scale):
    zl, win = lax.axis_index(ZL), lax.axis_index(WIN)
    squares = (s0[...] + s1[...]) + (s2[...] + s3[...])
    at = slice(PACKED, PACKED + 1)
    alphas = [u1_ref[0, SQUARES : SQUARES + 1], u2_ref[0, SQUARES : SQUARES + 1], norm_of(squares[0:1])]
    betas = [v0_ref[at], v1_ref[at], v2_ref[at]]
    rights = [ref[:PACKED] / a for ref, a in zip((v0_ref, v1_ref, v2_ref), alphas)]
    phi_bar, rho_bar = betas[0], alphas[0]
    search, estimate = rights[0], jnp.zeros((PACKED, LANES), f32)
    for alpha, beta, right in zip(alphas[1:], betas[1:], rights[1:]):
        rho = jnp.sqrt(rho_bar * rho_bar + beta * beta)
        cosine, sine = rho_bar / rho, beta / rho
        theta = sine * alpha
        rho_bar = -cosine * alpha
        phi = cosine * phi_bar
        phi_bar = sine * phi_bar
        estimate = estimate + phi / rho * search
        search = right - theta / rho * search
    for value, ref in ((estimate, slip_ref), (search * scale, direction_ref)):
        rows_ref[...] = pltpu.roll(value, LANES - zl * 32, 1)
        for a in range(2):
            row = rows_ref[pl.ds(win * 2 + a, 1), :]
            for one in range(2):
                ref[2 * a + one : 2 * a + one + 1, :] = row[:, one * 64 : one * 64 + 32]
    own = u2_ref[lax.axis_index(STA)]
    other = image_ref[lax.axis_index((ZL, Y, ZH)) ^ 8, HALF : HALF + PARTS, :]
    for comp in range(COMP):
        rows = slice(2 * comp, 2 * comp + 2)
        for h in range(2):
            value = jnp.where(zl == h, own[rows], other[rows])
            misfit_ref[0, comp, :, h * LANES : (h + 1) * LANES] = value / betas[2] * phi_bar


def from_partners(array, axis, at=range(4)):
    held = {k: lax.ppermute(array, axis, [(at[i], at[i ^ k]) for i in range(4)]) for k in ORDER}
    return [held[k] for k in (1, 2, 3)]


def other_core(array):
    return lax.ppermute(array, C, [(0, 1), (1, 0)])


def add_cores(own_ref, other_ref, both_ref, sent_ref):
    both = own_ref[...] + other_ref[...]
    both_ref[...] = both
    sent_ref[...] = both.astype(bf16)
    squares = both[0, SQUARES : SQUARES + 1]
    sent_ref[0, SQUARES + 1 :, :] = (squares - squares.astype(bf16).astype(f32)).astype(bf16)


def along_x(array):
    side = lax.ppermute(array, (X, C), [(x * 2 + c, (x ^ (1, 3)[c]) * 2 + c) for x in range(4) for c in range(2)])
    across = lax.ppermute(array, X, [(x, x ^ 2) for x in range(4)])
    return [across, side, other_core(side)]


def data_over_patches(array):
    both, sent = call(add_cores, [(array.shape, f32), (array.shape, bf16)], array, other_core(array))
    return [both, *along_x(sent)]


def squares_over_patches(array):
    both = array + other_core(array)
    return [both, *along_x(both)]


def summed_over_frequencies(buf):
    return lax.all_to_all(buf, (ZL, Y, ZH), 0, 0, tiled=True)


def local(green, records, onsets, mask):
    packed = pack(mask, green, records).reshape(16, ROWS, LANES)
    packed, onset_rows = lax.optimization_barrier((packed, onsets.T[None]))
    arrived = lax.all_to_all(packed, STA, 0, 0, tiled=True)
    rows = jnp.concatenate([onset_rows, *from_partners(onset_rows, Y)], axis=0)
    gathered = jnp.stack([rows, *from_partners(rows, (ZL, ZH), (0, 2, 1, 3))])
    head, tail = ((SPLIT, LANES, LANES), f32), ((PACKED - SPLIT, LANES, LANES), f32)
    tables = call(table_body, [head, head], gathered)

    buf_shape, data_shape, right_shape = ((16, IMAGE, LANES), f32), ((16, 8, LANES), f32), ((IMAGE, LANES), f32)

    def forward_call(first, *args):
        return pl.pallas_call(
            functools.partial(forward, first),
            in_specs=[VMEM] * len(args),
            out_specs=[VMEM] * 2,
            out_shape=[jax.ShapeDtypeStruct(*data_shape), jax.ShapeDtypeStruct(*right_shape)],
            compiler_params=PARAMS,
            cost_estimate=pl.CostEstimate(flops=2_000_000, bytes_accessed=4_000_000, transcendentals=0),
        )(*args)

    buf, u0, *rest = call(first_adjoint, [buf_shape, data_shape, tail, tail], arrived, *tables, gathered)
    base = (arrived, *tables, *rest)
    data, v0 = forward_call(True, *base, summed_over_frequencies(buf))
    buf, u1 = call(next_adjoint, [buf_shape, data_shape], *base, *data_over_patches(data), u0, v0)
    data, v1 = forward_call(False, *base, summed_over_frequencies(buf), v0, u1)
    buf, u2 = call(next_adjoint, [buf_shape, data_shape], *base, *data_over_patches(data), u1, v1)
    image = summed_over_frequencies(buf)
    v2, ss = call(last_right, [right_shape, ((8, LANES), f32)], image, v1, u2)
    scale = math.sqrt(512 * 32)
    slip, direction, misfit = call(
        functools.partial(finish, scale=scale),
        [((4, 32), f32), ((4, 32), f32), ((1, COMP, 2, 256), f32)],
        *squares_over_patches(ss), v0, v1, v2, u1, u2, image,
        scratch=[pltpu.VMEM((PACKED, LANES), f32)],
    )
    return slip.T, direction.T, misfit


def solution(mesh):
    finer = Mesh(mesh.devices.reshape(4, 2, 2, 4, 2), (X, ZL, C, Y, ZH))
    return jax.shard_map(
        local,
        mesh=finer,
        in_specs=(P(STA, None, None, None, WIN), P(STA, None, None, WIN), P(STA, WIN), P(STA, None)),
        out_specs=(P(STA, WIN), P(STA, WIN), P(STA, None, None, WIN)),
        check_vma=False,
    )
```

```python
import functools
import math

import jax
import jax.numpy as jnp
from jax import lax
from jax.experimental import pallas as pl
from jax.experimental.pallas import tpu as pltpu
from jax.sharding import Mesh
from jax.sharding import PartitionSpec as P

X, ZL, C, Y, ZH = "x", "zl", "core", "y", "zh"
STA = (X, ZL, C)
WIN = (Y, ZH)
SAMPLES = 4096
LANES = 128
COMP = 3
PARTS = 2 * COMP
PATCHES = 64
GREEN_ROWS = PARTS * PATCHES
TERMS = 2
ROWS = GREEN_ROWS + 8 * TERMS
PACKED = 16
IMAGE = 24
HALF = PACKED + 1
SQUARES = 6
f32, bf16 = jnp.float32, jnp.bfloat16
VMEM = pl.BlockSpec(memory_space=pltpu.VMEM)
HBM = pl.BlockSpec(memory_space=pltpu.HBM)
UNROLL = 4
ORDER = (3, 1, 2)
SPLIT = 14
PARAMS = pltpu.CompilerParams(vmem_limit_bytes=16 << 20)


def call(body, outs, *args, scratch=()):
    return pl.pallas_call(
        body,
        in_specs=[VMEM] * len(args),
        out_specs=[VMEM] * len(outs),
        out_shape=[jax.ShapeDtypeStruct(s, d) for s, d in outs],
        scratch_shapes=list(scratch),
        compiler_params=PARAMS,
        cost_estimate=pl.CostEstimate(flops=2_000_000, bytes_accessed=4_000_000, transcendentals=0),
    )(*args)


def pack_body(mask_hbm, green_hbm, rec_hbm, out_hbm, mask_ref, green_ref, rec_ref, out_ref, rows, in_sems, out_sems):
    reads = [pltpu.make_async_copy(green_hbm.at[0, k // 2, k % 2], green_ref.at[k], in_sems.at[k]) for k in range(PARTS)]
    reads.append(pltpu.make_async_copy(rec_hbm.at[0], rec_ref, in_sems.at[PARTS]))
    reads.append(pltpu.make_async_copy(mask_hbm, mask_ref, in_sems.at[PARTS + 1]))
    for read in reads[PARTS:] + reads[:PARTS]:
        read.start()
    reads[PARTS + 1].wait()
    reads[PARTS].wait()
    rows[...] = jnp.zeros_like(rows)
    for comp in range(COMP):
        rows[2 * comp : 2 * comp + 2, :] = jnp.where(mask_ref[0, comp] != 0, rec_ref[comp], 0.0)
    for half in range(2):
        rest = rows[:, half * LANES : (half + 1) * LANES]
        for term in range(TERMS):
            piece = rest.astype(bf16)
            rest = rest - piece.astype(f32)
            at = GREEN_ROWS + 8 * term
            for x in range(4):
                for c in range(2):
                    out_ref[x, half, c, at : at + 8, :] = piece
    writes = []
    for k in range(PARTS + 1):
        if k < PARTS:
            used = mask_ref[0, k // 2] != 0
            reads[k].wait()
            for x in range(4):
                for zl in range(2):
                    for c in range(2):
                        at = x * 128 + zl * 64 + c * 32
                        block = green_ref[k, at : at + 32, :]
                        block = jnp.where(used, block, jnp.zeros_like(block))
                        to = k * PATCHES + zl * 32
                        for half in range(2):
                            out_ref[x, half, c, to : to + 32, :] = block[:, half * LANES : (half + 1) * LANES]
        span = pl.ds(k * PATCHES, PATCHES if k < PARTS else 8 * TERMS)
        write = pltpu.make_async_copy(out_ref.at[:, :, :, span], out_hbm.at[:, :, :, span], out_sems.at[k])
        write.start()
        writes.append(write)
    for write in writes:
        write.wait()


def pack(mask, green, records):
    held = (4, 2, 2, ROWS, LANES)
    return pl.pallas_call(
        pack_body,
        in_specs=[HBM] * 3,
        out_specs=HBM,
        out_shape=jax.ShapeDtypeStruct(held, bf16),
        scratch_shapes=[
            pltpu.SMEM((1, COMP), jnp.int32),
            pltpu.VMEM((PARTS, 512, 256), bf16),
            pltpu.VMEM((COMP, 2, 256), f32),
            pltpu.VMEM(held, bf16),
            pltpu.VMEM((8, 256), f32),
            pltpu.SemaphoreType.DMA((PARTS + 2,)),
            pltpu.SemaphoreType.DMA((PARTS + 1,)),
        ],
        cost_estimate=pl.CostEstimate(flops=4_000_000, bytes_accessed=4_000_000, transcendentals=0),
    )(mask, green, records)


def fill_tables(onset_ref, first_pair, last_pair, cos_ref, sin_ref):
    y, z = lax.axis_index(Y), lax.axis_index(ZH) * 2 + lax.axis_index(ZL)
    first = lax.axis_index(WIN) * 256 + lax.axis_index(ZL) * LANES
    freq = lax.broadcasted_iota(jnp.int32, (LANES, LANES), 0) + first
    for pair in range(first_pair, last_pair):
        block, a = pair // 2, pair % 2
        pieces = [onset_ref[z ^ (block % 2 * 2 + zl), y ^ (block // 2)] for zl in range(2)]
        onset = jnp.concatenate([pieces[zl][2 * a + one : 2 * a + one + 1] for one in range(2) for zl in range(2)], axis=1)
        turns = onset * freq + SAMPLES // 8
        quarter = lax.shift_right_logical(turns, 10) & 3
        angle = ((turns & (SAMPLES // 4 - 1)) - SAMPLES // 8).astype(f32) * (2.0 * math.pi / SAMPLES)
        t = angle * angle
        s = angle * (1.0 + t * (-1 / 6 + t * (1 / 120 + t * (-1 / 5040 + t * (1 / 362880)))))
        c = 1.0 + t * (-0.5 + t * (1 / 24 + t * (-1 / 720 + t * (1 / 40320 + t * (-1 / 3628800)))))
        odd = (quarter & 1) == 1
        cosine = jnp.where(odd, s, c)
        sine = jnp.where(odd, c, s)
        cos_ref[pair - first_pair] = jnp.where((quarter == 1) | (quarter == 2), -cosine, cosine)
        sin_ref[pair - first_pair] = jnp.where(quarter >= 2, -sine, sine)


def table_body(onset_ref, cos_ref, sin_ref):
    fill_tables(onset_ref, 0, SPLIT, cos_ref, sin_ref)


def tables_of(refs):
    cos_a, sin_a, cos_b, sin_b = refs
    return lambda pair: (cos_a[pair], sin_a[pair]) if pair < SPLIT else (cos_b[pair - SPLIT], sin_b[pair - SPLIT])


def model_to_data(model_ref, ss, green_ref, tables, data_ref):
    re = jnp.zeros((LANES, LANES), f32)
    im = jnp.zeros((LANES, LANES), f32)
    for pair in range(PACKED):
        cosine, sine = tables(pair)
        v = model_ref[pair : pair + 1, :]
        re = re + v * cosine
        im = im - v * sine
    re, im = jnp.transpose(re, (1, 0)), jnp.transpose(im, (1, 0))
    re, im = re[:PATCHES] + re[PATCHES:], im[:PATCHES] + im[PATCHES:]
    zero = jnp.zeros((2, LANES), f32)

    def station(s, carry):
        for comp in range(COMP):
            at = 2 * comp * PATCHES
            g_re = green_ref[s, at : at + PATCHES, :].astype(f32)
            g_im = green_ref[s, at + PATCHES : at + 2 * PATCHES, :].astype(f32)
            data_ref[s, 2 * comp : 2 * comp + 1, :] = jnp.sum(g_re * re - g_im * im, axis=0, keepdims=True)
            data_ref[s, 2 * comp + 1 : 2 * comp + 2, :] = jnp.sum(g_re * im + g_im * re, axis=0, keepdims=True)
        data_ref[s, SQUARES:, :] = zero
        return carry

    lax.fori_loop(0, 16, station, 0, unroll=UNROLL)
    data_ref[0, SQUARES : SQUARES + 1, :] = ss


def data_to_model(u_ref, green_ref, tables, buf_ref, image_ref):
    def station(s, carry):
        q_re, q_im = carry
        for comp in range(COMP):
            at = 2 * comp * PATCHES
            g_re = green_ref[s, at : at + PATCHES, :].astype(f32)
            g_im = green_ref[s, at + PATCHES : at + 2 * PATCHES, :].astype(f32)
            u_re = u_ref[s, 2 * comp : 2 * comp + 1, :]
            u_im = u_ref[s, 2 * comp + 1 : 2 * comp + 2, :]
            q_re = q_re + (g_re * u_re + g_im * u_im)
            q_im = q_im + (g_re * u_im - g_im * u_re)
        return q_re, q_im

    zero = jnp.zeros((PATCHES, LANES), f32)
    q_re, q_im = lax.fori_loop(0, 16, station, (zero, zero), unroll=UNROLL)
    q_re, q_im = (jnp.transpose(jnp.concatenate([q, q], axis=0), (1, 0)) for q in (q_re, q_im))
    for pair in range(PACKED):
        cosine, sine = tables(pair)
        image_ref[pair : pair + 1, :] = jnp.sum(cosine * q_re - sine * q_im, axis=0, keepdims=True)
    used = lax.broadcasted_iota(jnp.int32, (16, 8, LANES), 1) < PARTS
    u = jnp.where(used, u_ref[...], 0.0)
    ss = jnp.sum(jnp.sum(u * u, axis=0), axis=0, keepdims=True)
    image_ref[PACKED:, :] = jnp.broadcast_to(ss, (IMAGE - PACKED, LANES))
    if buf_ref.dtype == bf16:
        image_ref[HALF : HALF + 1, :] = ss - ss.astype(bf16).astype(f32)
    else:
        image_ref[HALF : HALF + PARTS, :] = u_ref[lax.axis_index(STA) ^ 2, :PARTS, :]
    image = image_ref[...].astype(buf_ref.dtype)
    for d in range(16):
        buf_ref[d] = image


def first_adjoint(green_ref, cos_a, sin_a, onset_ref, buf_ref, u_ref, cos_b, sin_b, image_ref):
    fill_tables(onset_ref, SPLIT, PACKED, cos_b, sin_b)
    for s in range(16):
        terms = [green_ref[s, GREEN_ROWS + 8 * t : GREEN_ROWS + 8 * t + 8, :].astype(f32) for t in range(TERMS)]
        u_ref[s] = sum(terms)
    data_to_model(u_ref, green_ref, tables_of((cos_a, sin_a, cos_b, sin_b)), buf_ref, image_ref)


def norm_of(row):
    return jnp.broadcast_to(jnp.sqrt(jnp.sum(row, axis=1, keepdims=True)), (1, LANES))


def next_adjoint(green_ref, t0, t1, t2, t3, d0, d1, d2, d3, left_ref, right_ref, buf_ref, u_ref, image_ref):
    data = (d0[...] + d1[...].astype(f32)) + (d2[...].astype(f32) + d3[...].astype(f32))
    alpha = norm_of(data[0, SQUARES : SQUARES + 1] + data[0, SQUARES + 1 :])
    beta = right_ref[PACKED : PACKED + 1]
    u_ref[...] = data / alpha[None] - alpha[None] * (left_ref[...] / beta[None])
    u_ref[0, SQUARES : SQUARES + 1, :] = alpha
    data_to_model(u_ref, green_ref, tables_of((t0, t1, t2, t3)), buf_ref, image_ref)


def new_right(image_ref, right_ref, prev_ref, left_ref):
    image = jnp.sum(image_ref[...].astype(f32), axis=0)
    squares = image[PACKED : PACKED + 1]
    if image_ref.dtype == bf16:
        squares = squares + image[HALF : HALF + 1]
    beta = norm_of(squares)
    right = image[:PACKED] / beta
    if prev_ref is not None:
        right = right - beta * (prev_ref[:PACKED] / left_ref[0, SQUARES : SQUARES + 1])
    right_ref[:PACKED] = right
    right_ref[PACKED:] = jnp.broadcast_to(beta, (IMAGE - PACKED, LANES))
    return jnp.sum(right * right, axis=0, keepdims=True)


def forward(first, green_ref, t0, t1, t2, t3, image_ref, *refs):
    prev_ref, left_ref, data_ref, right_ref = ((None, None) + refs) if first else refs
    ss = new_right(image_ref, right_ref, prev_ref, left_ref)
    model_to_data(right_ref, ss, green_ref, tables_of((t0, t1, t2, t3)), data_ref)


def last_right(image_ref, prev_ref, left_ref, right_ref, ss_ref):
    ss = new_right(image_ref, right_ref, prev_ref, left_ref)
    ss_ref[...] = jnp.broadcast_to(ss, (8, LANES))


def finish(s0, s1, s2, s3, v0_ref, v1_ref, v2_ref, u1_ref, u2_ref, image_ref, slip_ref, direction_ref, misfit_ref, rows_ref, scale):
    zl, win = lax.axis_index(ZL), lax.axis_index(WIN)
    squares = (s0[...] + s1[...]) + (s2[...] + s3[...])
    at = slice(PACKED, PACKED + 1)
    alphas = [u1_ref[0, SQUARES : SQUARES + 1], u2_ref[0, SQUARES : SQUARES + 1], norm_of(squares[0:1])]
    betas = [v0_ref[at], v1_ref[at], v2_ref[at]]
    rights = [ref[:PACKED] / a for ref, a in zip((v0_ref, v1_ref, v2_ref), alphas)]
    phi_bar, rho_bar = betas[0], alphas[0]
    search, estimate = rights[0], jnp.zeros((PACKED, LANES), f32)
    for alpha, beta, right in zip(alphas[1:], betas[1:], rights[1:]):
        rho = jnp.sqrt(rho_bar * rho_bar + beta * beta)
        cosine, sine = rho_bar / rho, beta / rho
        theta = sine * alpha
        rho_bar = -cosine * alpha
        phi = cosine * phi_bar
        phi_bar = sine * phi_bar
        estimate = estimate + phi / rho * search
        search = right - theta / rho * search
    for value, ref in ((estimate, slip_ref), (search * scale, direction_ref)):
        rows_ref[...] = pltpu.roll(value, LANES - zl * 32, 1)
        for a in range(2):
            row = rows_ref[pl.ds(win * 2 + a, 1), :]
            for one in range(2):
                ref[2 * a + one : 2 * a + one + 1, :] = row[:, one * 64 : one * 64 + 32]
    own = u2_ref[lax.axis_index(STA)]
    other = image_ref[lax.axis_index((ZL, Y, ZH)) ^ 8, HALF : HALF + PARTS, :]
    for comp in range(COMP):
        rows = slice(2 * comp, 2 * comp + 2)
        for h in range(2):
            value = jnp.where(zl == h, own[rows], other[rows])
            misfit_ref[0, comp, :, h * LANES : (h + 1) * LANES] = value / betas[2] * phi_bar


def from_partners(array, axis, at=range(4)):
    held = {k: lax.ppermute(array, axis, [(at[i], at[i ^ k]) for i in range(4)]) for k in ORDER}
    return [held[k] for k in (1, 2, 3)]


def other_core(array):
    return lax.ppermute(array, C, [(0, 1), (1, 0)])


def add_cores(own_ref, other_ref, both_ref, sent_ref):
    both = own_ref[...] + other_ref[...]
    both_ref[...] = both
    sent_ref[...] = both.astype(bf16)
    squares = both[0, SQUARES : SQUARES + 1]
    sent_ref[0, SQUARES + 1 :, :] = (squares - squares.astype(bf16).astype(f32)).astype(bf16)


def along_x(array):
    side = lax.ppermute(array, (X, C), [(x * 2 + c, (x ^ (1, 3)[c]) * 2 + c) for x in range(4) for c in range(2)])
    across = lax.ppermute(array, X, [(x, x ^ 2) for x in range(4)])
    return [across, side, other_core(side)]


def data_over_patches(array):
    both, sent = call(add_cores, [(array.shape, f32), (array.shape, bf16)], array, other_core(array))
    return [both, *along_x(sent)]


def squares_over_patches(array):
    both = array + other_core(array)
    return [both, *along_x(both)]


def summed_over_frequencies(buf):
    return lax.all_to_all(buf, (ZL, Y, ZH), 0, 0, tiled=True)


def local(green, records, onsets, mask):
    packed = pack(mask, green, records).reshape(16, ROWS, LANES)
    packed, onset_rows = lax.optimization_barrier((packed, onsets.T[None]))
    arrived = lax.all_to_all(packed, STA, 0, 0, tiled=True)
    rows = jnp.concatenate([onset_rows, *from_partners(onset_rows, Y)], axis=0)
    gathered = jnp.stack([rows, *from_partners(rows, (ZL, ZH), (0, 2, 1, 3))])
    head, tail = ((SPLIT, LANES, LANES), f32), ((PACKED - SPLIT, LANES, LANES), f32)
    tables = call(table_body, [head, head], gathered)

    sent_shape, buf_shape = ((16, IMAGE, LANES), bf16), ((16, IMAGE, LANES), f32)
    held = [pltpu.VMEM((IMAGE, LANES), f32)]
    data_shape, right_shape = ((16, 8, LANES), f32), ((IMAGE, LANES), f32)

    def forward_call(first, *args):
        return pl.pallas_call(
            functools.partial(forward, first),
            in_specs=[VMEM] * len(args),
            out_specs=[VMEM] * 2,
            out_shape=[jax.ShapeDtypeStruct(*data_shape), jax.ShapeDtypeStruct(*right_shape)],
            compiler_params=PARAMS,
            cost_estimate=pl.CostEstimate(flops=2_000_000, bytes_accessed=4_000_000, transcendentals=0),
        )(*args)

    buf, u0, *rest = call(first_adjoint, [sent_shape, data_shape, tail, tail], arrived, *tables, gathered, scratch=held)
    base = (arrived, *tables, *rest)
    data, v0 = forward_call(True, *base, summed_over_frequencies(buf))
    buf, u1 = call(next_adjoint, [sent_shape, data_shape], *base, *data_over_patches(data), u0, v0, scratch=held)
    data, v1 = forward_call(False, *base, summed_over_frequencies(buf), v0, u1)
    buf, u2 = call(next_adjoint, [buf_shape, data_shape], *base, *data_over_patches(data), u1, v1, scratch=held)
    image = summed_over_frequencies(buf)
    v2, ss = call(last_right, [right_shape, ((8, LANES), f32)], image, v1, u2)
    scale = math.sqrt(512 * 32)
    slip, direction, misfit = call(
        functools.partial(finish, scale=scale),
        [((4, 32), f32), ((4, 32), f32), ((1, COMP, 2, 256), f32)],
        *squares_over_patches(ss), v0, v1, v2, u1, u2, image,
        scratch=[pltpu.VMEM((PACKED, LANES), f32)],
    )
    return slip.T, direction.T, misfit


def solution(mesh):
    finer = Mesh(mesh.devices.reshape(4, 2, 2, 4, 2), (X, ZL, C, Y, ZH))
    return jax.shard_map(
        local,
        mesh=finer,
        in_specs=(P(STA, None, None, None, WIN), P(STA, None, None, WIN), P(STA, WIN), P(STA, None)),
        out_specs=(P(STA, WIN), P(STA, WIN), P(STA, None, None, WIN)),
        check_vma=False,
    )
```

```python
import functools
import math

import jax
import jax.numpy as jnp
from jax import lax
from jax.experimental import pallas as pl
from jax.experimental.pallas import tpu as pltpu
from jax.sharding import Mesh
from jax.sharding import PartitionSpec as P

X, ZL, C, Y, ZH = "x", "zl", "core", "y", "zh"
STA = (X, ZL, C)
WIN = (Y, ZH)
SAMPLES = 4096
LANES = 128
COMP = 3
PARTS = 2 * COMP
PATCHES = 64
GREEN_ROWS = PARTS * PATCHES
TERMS = 2
ROWS = GREEN_ROWS + 8 * TERMS
PACKED = 16
IMAGE = 24
HALF = PACKED + 2
LAST_IMAGE = HALF + 14
SQUARES = 6
f32, bf16 = jnp.float32, jnp.bfloat16
VMEM = pl.BlockSpec(memory_space=pltpu.VMEM)
HBM = pl.BlockSpec(memory_space=pltpu.HBM)
UNROLL = 4
ORDER = (3, 1, 2)
SPLIT = 14
PARAMS = pltpu.CompilerParams(vmem_limit_bytes=16 << 20)


def call(body, outs, *args, scratch=()):
    return pl.pallas_call(
        body,
        in_specs=[VMEM] * len(args),
        out_specs=[VMEM] * len(outs),
        out_shape=[jax.ShapeDtypeStruct(s, d) for s, d in outs],
        scratch_shapes=list(scratch),
        compiler_params=PARAMS,
        cost_estimate=pl.CostEstimate(flops=2_000_000, bytes_accessed=4_000_000, transcendentals=0),
    )(*args)


def pack_body(mask_hbm, green_hbm, rec_hbm, out_hbm, mask_ref, green_ref, rec_ref, out_ref, rows, in_sems, out_sems):
    reads = [pltpu.make_async_copy(green_hbm.at[0, k // 2, k % 2], green_ref.at[k], in_sems.at[k]) for k in range(PARTS)]
    reads.append(pltpu.make_async_copy(rec_hbm.at[0], rec_ref, in_sems.at[PARTS]))
    reads.append(pltpu.make_async_copy(mask_hbm, mask_ref, in_sems.at[PARTS + 1]))
    for read in reads[PARTS:] + reads[:PARTS]:
        read.start()
    reads[PARTS + 1].wait()
    reads[PARTS].wait()
    rows[...] = jnp.zeros_like(rows)
    for comp in range(COMP):
        rows[2 * comp : 2 * comp + 2, :] = jnp.where(mask_ref[0, comp] != 0, rec_ref[comp], 0.0)
    for half in range(2):
        rest = rows[:, half * LANES : (half + 1) * LANES]
        for term in range(TERMS):
            piece = rest.astype(bf16)
            rest = rest - piece.astype(f32)
            at = GREEN_ROWS + 8 * term
            for x in range(4):
                for c in range(2):
                    out_ref[x, half, c, at : at + 8, :] = piece
    writes = []
    for k in range(PARTS + 1):
        if k < PARTS:
            used = mask_ref[0, k // 2] != 0
            reads[k].wait()
            for x in range(4):
                for zl in range(2):
                    for c in range(2):
                        at = x * 128 + zl * 64 + c * 32
                        block = green_ref[k, at : at + 32, :]
                        block = jnp.where(used, block, jnp.zeros_like(block))
                        to = k * PATCHES + zl * 32
                        for half in range(2):
                            out_ref[x, half, c, to : to + 32, :] = block[:, half * LANES : (half + 1) * LANES]
        span = pl.ds(k * PATCHES, PATCHES if k < PARTS else 8 * TERMS)
        write = pltpu.make_async_copy(out_ref.at[:, :, :, span], out_hbm.at[:, :, :, span], out_sems.at[k])
        write.start()
        writes.append(write)
    for write in writes:
        write.wait()


def pack(mask, green, records):
    held = (4, 2, 2, ROWS, LANES)
    return pl.pallas_call(
        pack_body,
        in_specs=[HBM] * 3,
        out_specs=HBM,
        out_shape=jax.ShapeDtypeStruct(held, bf16),
        scratch_shapes=[
            pltpu.SMEM((1, COMP), jnp.int32),
            pltpu.VMEM((PARTS, 512, 256), bf16),
            pltpu.VMEM((COMP, 2, 256), f32),
            pltpu.VMEM(held, bf16),
            pltpu.VMEM((8, 256), f32),
            pltpu.SemaphoreType.DMA((PARTS + 2,)),
            pltpu.SemaphoreType.DMA((PARTS + 1,)),
        ],
        cost_estimate=pl.CostEstimate(flops=4_000_000, bytes_accessed=4_000_000, transcendentals=0),
    )(mask, green, records)


def fill_tables(onset_ref, first_pair, last_pair, cos_ref, sin_ref):
    y, z = lax.axis_index(Y), lax.axis_index(ZH) * 2 + lax.axis_index(ZL)
    first = lax.axis_index(WIN) * 256 + lax.axis_index(ZL) * LANES
    freq = lax.broadcasted_iota(jnp.int32, (LANES, LANES), 0) + first
    for pair in range(first_pair, last_pair):
        block, a = pair // 2, pair % 2
        pieces = [onset_ref[z ^ (block % 2 * 2 + zl), y ^ (block // 2)] for zl in range(2)]
        onset = jnp.concatenate([pieces[zl][2 * a + one : 2 * a + one + 1] for one in range(2) for zl in range(2)], axis=1)
        turns = onset * freq + SAMPLES // 8
        quarter = lax.shift_right_logical(turns, 10) & 3
        angle = ((turns & (SAMPLES // 4 - 1)) - SAMPLES // 8).astype(f32) * (2.0 * math.pi / SAMPLES)
        t = angle * angle
        s = angle * (1.0 + t * (-1 / 6 + t * (1 / 120 + t * (-1 / 5040 + t * (1 / 362880)))))
        c = 1.0 + t * (-0.5 + t * (1 / 24 + t * (-1 / 720 + t * (1 / 40320 + t * (-1 / 3628800)))))
        odd = (quarter & 1) == 1
        cosine = jnp.where(odd, s, c)
        sine = jnp.where(odd, c, s)
        cos_ref[pair - first_pair] = jnp.where((quarter == 1) | (quarter == 2), -cosine, cosine)
        sin_ref[pair - first_pair] = jnp.where(quarter >= 2, -sine, sine)


def table_body(onset_ref, cos_ref, sin_ref):
    fill_tables(onset_ref, 0, SPLIT, cos_ref, sin_ref)


def tables_of(refs):
    cos_a, sin_a, cos_b, sin_b = refs
    return lambda pair: (cos_a[pair], sin_a[pair]) if pair < SPLIT else (cos_b[pair - SPLIT], sin_b[pair - SPLIT])


def model_to_data(model_ref, ss, green_ref, tables, data_ref):
    re = jnp.zeros((LANES, LANES), f32)
    im = jnp.zeros((LANES, LANES), f32)
    for pair in range(PACKED):
        cosine, sine = tables(pair)
        v = model_ref[pair : pair + 1, :]
        re = re + v * cosine
        im = im - v * sine
    re, im = jnp.transpose(re, (1, 0)), jnp.transpose(im, (1, 0))
    re, im = re[:PATCHES] + re[PATCHES:], im[:PATCHES] + im[PATCHES:]
    zero = jnp.zeros((2, LANES), f32)

    def station(s, carry):
        for comp in range(COMP):
            at = 2 * comp * PATCHES
            g_re = green_ref[s, at : at + PATCHES, :].astype(f32)
            g_im = green_ref[s, at + PATCHES : at + 2 * PATCHES, :].astype(f32)
            data_ref[s, 2 * comp : 2 * comp + 1, :] = jnp.sum(g_re * re - g_im * im, axis=0, keepdims=True)
            data_ref[s, 2 * comp + 1 : 2 * comp + 2, :] = jnp.sum(g_re * im + g_im * re, axis=0, keepdims=True)
        data_ref[s, SQUARES:, :] = zero
        return carry

    lax.fori_loop(0, 16, station, 0, unroll=UNROLL)
    data_ref[0, SQUARES : SQUARES + 1, :] = ss


def data_to_model(u_ref, green_ref, tables, buf_ref, image_ref):
    def station(s, carry):
        q_re, q_im = carry
        for comp in range(COMP):
            at = 2 * comp * PATCHES
            g_re = green_ref[s, at : at + PATCHES, :].astype(f32)
            g_im = green_ref[s, at + PATCHES : at + 2 * PATCHES, :].astype(f32)
            u_re = u_ref[s, 2 * comp : 2 * comp + 1, :]
            u_im = u_ref[s, 2 * comp + 1 : 2 * comp + 2, :]
            q_re = q_re + (g_re * u_re + g_im * u_im)
            q_im = q_im + (g_re * u_im - g_im * u_re)
        return q_re, q_im

    zero = jnp.zeros((PATCHES, LANES), f32)
    q_re, q_im = lax.fori_loop(0, 16, station, (zero, zero), unroll=UNROLL)
    q_re, q_im = (jnp.transpose(jnp.concatenate([q, q], axis=0), (1, 0)) for q in (q_re, q_im))
    for pair in range(PACKED):
        cosine, sine = tables(pair)
        image_ref[pair : pair + 1, :] = jnp.sum(cosine * q_re - sine * q_im, axis=0, keepdims=True)
    used = lax.broadcasted_iota(jnp.int32, (16, 8, LANES), 1) < PARTS
    u = jnp.where(used, u_ref[...], 0.0)
    ss = jnp.sum(jnp.sum(u * u, axis=0), axis=0, keepdims=True)
    image_ref[PACKED:, :] = jnp.broadcast_to(ss, (LAST_IMAGE - PACKED, LANES))
    image_ref[PACKED + 1 : PACKED + 2, :] = ss - ss.astype(bf16).astype(f32)
    if buf_ref.shape[1] > IMAGE:
        half = u_ref[lax.axis_index(STA) ^ 2, :PARTS, :]
        image_ref[HALF : HALF + PARTS, :] = half
        image_ref[HALF + 8 : HALF + 8 + PARTS, :] = half - half.astype(bf16).astype(f32)
    image = image_ref[: buf_ref.shape[1]].astype(bf16)
    for d in range(16):
        buf_ref[d] = image


def first_adjoint(green_ref, cos_a, sin_a, onset_ref, buf_ref, u_ref, cos_b, sin_b, image_ref):
    fill_tables(onset_ref, SPLIT, PACKED, cos_b, sin_b)
    for s in range(16):
        terms = [green_ref[s, GREEN_ROWS + 8 * t : GREEN_ROWS + 8 * t + 8, :].astype(f32) for t in range(TERMS)]
        u_ref[s] = sum(terms)
    data_to_model(u_ref, green_ref, tables_of((cos_a, sin_a, cos_b, sin_b)), buf_ref, image_ref)


def norm_of(row):
    return jnp.broadcast_to(jnp.sqrt(jnp.sum(row, axis=1, keepdims=True)), (1, LANES))


def next_adjoint(green_ref, t0, t1, t2, t3, d0, d1, d2, d3, left_ref, right_ref, buf_ref, u_ref, image_ref):
    data = (d0[...] + d1[...].astype(f32)) + (d2[...].astype(f32) + d3[...].astype(f32))
    alpha = norm_of(data[0, SQUARES : SQUARES + 1] + data[0, SQUARES + 1 :])
    beta = right_ref[PACKED : PACKED + 1]
    u_ref[...] = data / alpha[None] - alpha[None] * (left_ref[...] / beta[None])
    u_ref[0, SQUARES : SQUARES + 1, :] = alpha
    data_to_model(u_ref, green_ref, tables_of((t0, t1, t2, t3)), buf_ref, image_ref)


def new_right(image_ref, right_ref, prev_ref, left_ref):
    image = jnp.sum(image_ref[...].astype(f32), axis=0)
    beta = norm_of(image[PACKED : PACKED + 1] + image[PACKED + 1 : PACKED + 2])
    right = image[:PACKED] / beta
    if prev_ref is not None:
        right = right - beta * (prev_ref[:PACKED] / left_ref[0, SQUARES : SQUARES + 1])
    right_ref[:PACKED] = right
    right_ref[PACKED:] = jnp.broadcast_to(beta, (IMAGE - PACKED, LANES))
    return jnp.sum(right * right, axis=0, keepdims=True)


def forward(first, green_ref, t0, t1, t2, t3, image_ref, *refs):
    prev_ref, left_ref, data_ref, right_ref = ((None, None) + refs) if first else refs
    ss = new_right(image_ref, right_ref, prev_ref, left_ref)
    model_to_data(right_ref, ss, green_ref, tables_of((t0, t1, t2, t3)), data_ref)


def last_right(image_ref, prev_ref, left_ref, right_ref, ss_ref):
    ss = new_right(image_ref, right_ref, prev_ref, left_ref)
    ss_ref[...] = jnp.broadcast_to(ss, (8, LANES))


def own_block(value, ref, rows_ref):
    rows_ref[...] = pltpu.roll(value, LANES - lax.axis_index(ZL) * 32, 1)
    for a in range(2):
        row = rows_ref[pl.ds(lax.axis_index(WIN) * 2 + a, 1), :]
        for one in range(2):
            ref[2 * a + one : 2 * a + one + 1, :] = row[:, one * 64 : one * 64 + 32]


def settle(v0_ref, v1_ref, v2_ref, u1_ref, u2_ref, image_ref, slip_ref, misfit_ref, right_ref, search_ref, rows_ref):
    zl = lax.axis_index(ZL)
    at = slice(PACKED, PACKED + 1)
    alphas = [ref[0, SQUARES : SQUARES + 1] for ref in (u1_ref, u2_ref)]
    betas = [ref[at] for ref in (v0_ref, v1_ref, v2_ref)]
    rights = [ref[:PACKED] / a for ref, a in zip((v0_ref, v1_ref), alphas)]
    phi_bar, rho_bar = betas[0], alphas[0]
    search, estimate = rights[0], jnp.zeros((PACKED, LANES), f32)
    for sweep in range(2):
        beta = betas[sweep + 1]
        rho = jnp.sqrt(rho_bar * rho_bar + beta * beta)
        cosine, sine = rho_bar / rho, beta / rho
        phi = cosine * phi_bar
        phi_bar = sine * phi_bar
        estimate = estimate + phi / rho * search
        if sweep == 0:
            rho_bar = -cosine * alphas[1]
            search = rights[1] - sine * alphas[1] / rho * search
        else:
            search = sine / rho * search
    own_block(estimate, slip_ref, rows_ref)
    own_block(v2_ref[:PACKED], right_ref, rows_ref)
    own_block(search, search_ref, rows_ref)
    own = u2_ref[lax.axis_index(STA)]
    source = lax.axis_index((ZL, Y, ZH)) ^ 8
    other = image_ref[source, HALF : HALF + PARTS, :].astype(f32) + image_ref[source, HALF + 8 : HALF + 8 + PARTS, :].astype(f32)
    for comp in range(COMP):
        rows = slice(2 * comp, 2 * comp + 2)
        for h in range(2):
            value = jnp.where(zl == h, own[rows], other[rows])
            misfit_ref[0, comp, :, h * LANES : (h + 1) * LANES] = value / betas[2] * phi_bar


def finish(s0, s1, s2, s3, right_ref, search_ref, direction_ref, scale):
    alpha = norm_of((s0[0:1] + s1[0:1]) + (s2[0:1] + s3[0:1]))[:, :32]
    direction_ref[...] = (right_ref[...] / alpha - alpha * search_ref[...]) * scale


def from_partners(array, axis, at=range(4)):
    held = {k: lax.ppermute(array, axis, [(at[i], at[i ^ k]) for i in range(4)]) for k in ORDER}
    return [held[k] for k in (1, 2, 3)]


def other_core(array):
    return lax.ppermute(array, C, [(0, 1), (1, 0)])


def add_cores(own_ref, other_ref, both_ref, sent_ref):
    both = own_ref[...] + other_ref[...]
    both_ref[...] = both
    sent_ref[...] = both.astype(bf16)
    squares = both[0, SQUARES : SQUARES + 1]
    sent_ref[0, SQUARES + 1 :, :] = (squares - squares.astype(bf16).astype(f32)).astype(bf16)


def along_x(array):
    side = lax.ppermute(array, (X, C), [(x * 2 + c, (x ^ (1, 3)[c]) * 2 + c) for x in range(4) for c in range(2)])
    across = lax.ppermute(array, X, [(x, x ^ 2) for x in range(4)])
    return [across, side, other_core(side)]


def data_over_patches(array):
    both, sent = call(add_cores, [(array.shape, f32), (array.shape, bf16)], array, other_core(array))
    return [both, *along_x(sent)]


def squares_over_patches(array):
    both = array + other_core(array)
    return [both, *along_x(both)]


def summed_over_frequencies(buf):
    return lax.all_to_all(buf, (ZL, Y, ZH), 0, 0, tiled=True)


def local(green, records, onsets, mask):
    packed = pack(mask, green, records).reshape(16, ROWS, LANES)
    packed, onset_rows = lax.optimization_barrier((packed, onsets.T[None]))
    arrived = lax.all_to_all(packed, STA, 0, 0, tiled=True)
    rows = jnp.concatenate([onset_rows, *from_partners(onset_rows, Y)], axis=0)
    gathered = jnp.stack([rows, *from_partners(rows, (ZL, ZH), (0, 2, 1, 3))])
    head, tail = ((SPLIT, LANES, LANES), f32), ((PACKED - SPLIT, LANES, LANES), f32)
    tables = call(table_body, [head, head], gathered)

    sent_shape, buf_shape = (((16, rows, LANES), bf16) for rows in (IMAGE, LAST_IMAGE))
    held = [pltpu.VMEM((LAST_IMAGE, LANES), f32)]
    data_shape, right_shape = ((16, 8, LANES), f32), ((IMAGE, LANES), f32)

    def forward_call(first, *args):
        return pl.pallas_call(
            functools.partial(forward, first),
            in_specs=[VMEM] * len(args),
            out_specs=[VMEM] * 2,
            out_shape=[jax.ShapeDtypeStruct(*data_shape), jax.ShapeDtypeStruct(*right_shape)],
            compiler_params=PARAMS,
            cost_estimate=pl.CostEstimate(flops=2_000_000, bytes_accessed=4_000_000, transcendentals=0),
        )(*args)

    buf, u0, *rest = call(first_adjoint, [sent_shape, data_shape, tail, tail], arrived, *tables, gathered, scratch=held)
    base = (arrived, *tables, *rest)
    data, v0 = forward_call(True, *base, summed_over_frequencies(buf))
    buf, u1 = call(next_adjoint, [sent_shape, data_shape], *base, *data_over_patches(data), u0, v0, scratch=held)
    data, v1 = forward_call(False, *base, summed_over_frequencies(buf), v0, u1)
    buf, u2 = call(next_adjoint, [buf_shape, data_shape], *base, *data_over_patches(data), u1, v1, scratch=held)
    image = summed_over_frequencies(buf)
    v2, ss = call(last_right, [right_shape, ((8, LANES), f32)], image, v1, u2)
    scale = math.sqrt(512 * 32)
    block = ((4, 32), f32)
    slip, misfit, right, search = call(
        settle, [block, ((1, COMP, 2, 256), f32), block, block], v0, v1, v2, u1, u2, image, scratch=[pltpu.VMEM((PACKED, LANES), f32)]
    )
    (direction,) = call(functools.partial(finish, scale=scale), [block], *squares_over_patches(ss), right, search)
    return slip.T, direction.T, misfit


def solution(mesh):
    finer = Mesh(mesh.devices.reshape(4, 2, 2, 4, 2), (X, ZL, C, Y, ZH))
    return jax.shard_map(
        local,
        mesh=finer,
        in_specs=(P(STA, None, None, None, WIN), P(STA, None, None, WIN), P(STA, WIN), P(STA, None)),
        out_specs=(P(STA, WIN), P(STA, WIN), P(STA, None, None, WIN)),
        check_vma=False,
    )
```

```python
import functools
import math

import jax
import jax.numpy as jnp
from jax import lax
from jax.experimental import pallas as pl
from jax.experimental.pallas import tpu as pltpu
from jax.sharding import Mesh
from jax.sharding import PartitionSpec as P

X, ZL, C, Y, ZH = "x", "zl", "core", "y", "zh"
STA = (X, ZL, C)
WIN = (Y, ZH)
SAMPLES = 4096
LANES = 128
COMP = 3
PARTS = 2 * COMP
PATCHES = 64
GREEN_ROWS = PARTS * PATCHES
TERMS = 2
ROWS = GREEN_ROWS + 8 * TERMS
PACKED = 16
IMAGE = 24
HALF = PACKED + 2
LAST_IMAGE = HALF + 14
SQUARES = 6
f32, bf16 = jnp.float32, jnp.bfloat16
VMEM = pl.BlockSpec(memory_space=pltpu.VMEM)
HBM = pl.BlockSpec(memory_space=pltpu.HBM)
UNROLL = 4
ORDER = (3, 1, 2)
SPLIT = 14
PARAMS = pltpu.CompilerParams(vmem_limit_bytes=16 << 20)


def call(body, outs, *args, scratch=()):
    return pl.pallas_call(
        body,
        in_specs=[VMEM] * len(args),
        out_specs=[VMEM] * len(outs),
        out_shape=[jax.ShapeDtypeStruct(s, d) for s, d in outs],
        scratch_shapes=list(scratch),
        compiler_params=PARAMS,
        cost_estimate=pl.CostEstimate(flops=2_000_000, bytes_accessed=4_000_000, transcendentals=0),
    )(*args)


def pack_body(mask_hbm, green_hbm, rec_hbm, out_hbm, mask_ref, green_ref, rec_ref, out_ref, rows, in_sems, out_sems):
    reads = [pltpu.make_async_copy(green_hbm.at[0, k // 2, k % 2], green_ref.at[k], in_sems.at[k]) for k in range(PARTS)]
    reads.append(pltpu.make_async_copy(rec_hbm.at[0], rec_ref, in_sems.at[PARTS]))
    reads.append(pltpu.make_async_copy(mask_hbm, mask_ref, in_sems.at[PARTS + 1]))
    for read in reads[PARTS:] + reads[:PARTS]:
        read.start()
    reads[PARTS + 1].wait()
    reads[PARTS].wait()
    rows[...] = jnp.zeros_like(rows)
    for comp in range(COMP):
        rows[2 * comp : 2 * comp + 2, :] = jnp.where(mask_ref[0, comp] != 0, rec_ref[comp], 0.0)
    for half in range(2):
        rest = rows[:, half * LANES : (half + 1) * LANES]
        for term in range(TERMS):
            piece = rest.astype(bf16)
            rest = rest - piece.astype(f32)
            at = GREEN_ROWS + 8 * term
            for x in range(4):
                for c in range(2):
                    out_ref[x, half, c, at : at + 8, :] = piece
    writes = []
    for k in range(PARTS + 1):
        if k < PARTS:
            used = mask_ref[0, k // 2] != 0
            reads[k].wait()
            for x in range(4):
                for zl in range(2):
                    for c in range(2):
                        at = x * 128 + zl * 64 + c * 32
                        block = green_ref[k, at : at + 32, :]
                        block = jnp.where(used, block, jnp.zeros_like(block))
                        to = k * PATCHES + zl * 32
                        for half in range(2):
                            out_ref[x, half, c, to : to + 32, :] = block[:, half * LANES : (half + 1) * LANES]
        span = pl.ds(k * PATCHES, PATCHES if k < PARTS else 8 * TERMS)
        write = pltpu.make_async_copy(out_ref.at[:, :, :, span], out_hbm.at[:, :, :, span], out_sems.at[k])
        write.start()
        writes.append(write)
    for write in writes:
        write.wait()


def pack(mask, green, records):
    held = (4, 2, 2, ROWS, LANES)
    return pl.pallas_call(
        pack_body,
        in_specs=[HBM] * 3,
        out_specs=HBM,
        out_shape=jax.ShapeDtypeStruct(held, bf16),
        scratch_shapes=[
            pltpu.SMEM((1, COMP), jnp.int32),
            pltpu.VMEM((PARTS, 512, 256), bf16),
            pltpu.VMEM((COMP, 2, 256), f32),
            pltpu.VMEM(held, bf16),
            pltpu.VMEM((8, 256), f32),
            pltpu.SemaphoreType.DMA((PARTS + 2,)),
            pltpu.SemaphoreType.DMA((PARTS + 1,)),
        ],
        cost_estimate=pl.CostEstimate(flops=4_000_000, bytes_accessed=4_000_000, transcendentals=0),
    )(mask, green, records)


def fill_tables(onset_ref, first_pair, last_pair, cos_ref, sin_ref):
    y, z = lax.axis_index(Y), lax.axis_index(ZH) * 2 + lax.axis_index(ZL)
    first = lax.axis_index(WIN) * 256 + lax.axis_index(ZL) * LANES
    freq = lax.broadcasted_iota(jnp.int32, (LANES, LANES), 0) + first
    for pair in range(first_pair, last_pair):
        block, a = pair // 2, pair % 2
        pieces = [onset_ref[z ^ (block % 2 * 2 + zl), y ^ (block // 2)] for zl in range(2)]
        onset = jnp.concatenate([pieces[zl][2 * a + one : 2 * a + one + 1] for one in range(2) for zl in range(2)], axis=1)
        turns = onset * freq + SAMPLES // 8
        quarter = lax.shift_right_logical(turns, 10) & 3
        angle = ((turns & (SAMPLES // 4 - 1)) - SAMPLES // 8).astype(f32) * (2.0 * math.pi / SAMPLES)
        t = angle * angle
        s = angle * (1.0 + t * (-1 / 6 + t * (1 / 120 + t * (-1 / 5040 + t * (1 / 362880)))))
        c = 1.0 + t * (-0.5 + t * (1 / 24 + t * (-1 / 720 + t * (1 / 40320 + t * (-1 / 3628800)))))
        odd = (quarter & 1) == 1
        cosine = jnp.where(odd, s, c)
        sine = jnp.where(odd, c, s)
        cos_ref[pair - first_pair] = jnp.where((quarter == 1) | (quarter == 2), -cosine, cosine)
        sin_ref[pair - first_pair] = jnp.where(quarter >= 2, -sine, sine)


def table_body(onset_ref, cos_ref, sin_ref):
    fill_tables(onset_ref, 0, SPLIT, cos_ref, sin_ref)


def tables_of(refs):
    cos_a, sin_a, cos_b, sin_b = refs
    return lambda pair: (cos_a[pair], sin_a[pair]) if pair < SPLIT else (cos_b[pair - SPLIT], sin_b[pair - SPLIT])


def model_to_data(model_ref, ss, green_ref, tables, data_ref):
    re = jnp.zeros((LANES, LANES), f32)
    im = jnp.zeros((LANES, LANES), f32)
    for pair in range(PACKED):
        cosine, sine = tables(pair)
        v = model_ref[pair : pair + 1, :]
        re = re + v * cosine
        im = im - v * sine
    re, im = jnp.transpose(re, (1, 0)), jnp.transpose(im, (1, 0))
    re, im = re[:PATCHES] + re[PATCHES:], im[:PATCHES] + im[PATCHES:]
    zero = jnp.zeros((2, LANES), f32)

    def station(s, carry):
        for comp in range(COMP):
            at = 2 * comp * PATCHES
            g_re = green_ref[s, at : at + PATCHES, :].astype(f32)
            g_im = green_ref[s, at + PATCHES : at + 2 * PATCHES, :].astype(f32)
            data_ref[s, 2 * comp : 2 * comp + 1, :] = jnp.sum(g_re * re - g_im * im, axis=0, keepdims=True)
            data_ref[s, 2 * comp + 1 : 2 * comp + 2, :] = jnp.sum(g_re * im + g_im * re, axis=0, keepdims=True)
        data_ref[s, SQUARES:, :] = zero
        return carry

    lax.fori_loop(0, 16, station, 0, unroll=UNROLL)
    data_ref[0, SQUARES : SQUARES + 1, :] = ss


def data_to_model(u_ref, green_ref, tables, buf_ref, image_ref):
    def station(s, carry):
        q_re, q_im = carry
        for comp in range(COMP):
            at = 2 * comp * PATCHES
            g_re = green_ref[s, at : at + PATCHES, :].astype(f32)
            g_im = green_ref[s, at + PATCHES : at + 2 * PATCHES, :].astype(f32)
            u_re = u_ref[s, 2 * comp : 2 * comp + 1, :]
            u_im = u_ref[s, 2 * comp + 1 : 2 * comp + 2, :]
            q_re = q_re + (g_re * u_re + g_im * u_im)
            q_im = q_im + (g_re * u_im - g_im * u_re)
        return q_re, q_im

    zero = jnp.zeros((PATCHES, LANES), f32)
    q_re, q_im = lax.fori_loop(0, 16, station, (zero, zero), unroll=UNROLL)
    q_re, q_im = (jnp.transpose(jnp.concatenate([q, q], axis=0), (1, 0)) for q in (q_re, q_im))
    for pair in range(PACKED):
        cosine, sine = tables(pair)
        image_ref[pair : pair + 1, :] = jnp.sum(cosine * q_re - sine * q_im, axis=0, keepdims=True)
    used = lax.broadcasted_iota(jnp.int32, (16, 8, LANES), 1) < PARTS
    u = jnp.where(used, u_ref[...], 0.0)
    ss = jnp.sum(jnp.sum(u * u, axis=0), axis=0, keepdims=True)
    image_ref[PACKED:, :] = jnp.broadcast_to(ss, (LAST_IMAGE - PACKED, LANES))
    image_ref[PACKED + 1 : PACKED + 2, :] = ss - ss.astype(bf16).astype(f32)
    if buf_ref.shape[1] > IMAGE:
        half = u_ref[lax.axis_index(STA) ^ 2, :PARTS, :]
        image_ref[HALF : HALF + PARTS, :] = half
        image_ref[HALF + 8 : HALF + 8 + PARTS, :] = half - half.astype(bf16).astype(f32)
    image = image_ref[: buf_ref.shape[1]].astype(bf16)
    for d in range(16):
        buf_ref[d] = image


def first_adjoint(green_ref, cos_a, sin_a, onset_ref, buf_ref, u_ref, cos_b, sin_b, image_ref):
    fill_tables(onset_ref, SPLIT, PACKED, cos_b, sin_b)
    for s in range(16):
        terms = [green_ref[s, GREEN_ROWS + 8 * t : GREEN_ROWS + 8 * t + 8, :].astype(f32) for t in range(TERMS)]
        u_ref[s] = sum(terms)
    data_to_model(u_ref, green_ref, tables_of((cos_a, sin_a, cos_b, sin_b)), buf_ref, image_ref)


def norm_of(row):
    return jnp.broadcast_to(jnp.sqrt(jnp.sum(row, axis=1, keepdims=True)), (1, LANES))


def next_adjoint(green_ref, t0, t1, t2, t3, d0, d1, d2, d3, left_ref, right_ref, buf_ref, u_ref, image_ref):
    data = (d0[...] + d1[...].astype(f32)) + (d2[...].astype(f32) + d3[...].astype(f32))
    alpha = norm_of(data[0, SQUARES : SQUARES + 1] + data[0, SQUARES + 1 :])
    beta = right_ref[PACKED : PACKED + 1]
    u_ref[...] = data / alpha[None] - alpha[None] * (left_ref[...] / beta[None])
    u_ref[0, SQUARES : SQUARES + 1, :] = alpha
    data_to_model(u_ref, green_ref, tables_of((t0, t1, t2, t3)), buf_ref, image_ref)


def new_right(image_ref, right_ref, prev_ref, left_ref):
    image = jnp.sum(image_ref[...].astype(f32), axis=0)
    beta = norm_of(image[PACKED : PACKED + 1] + image[PACKED + 1 : PACKED + 2])
    right = image[:PACKED] / beta
    if prev_ref is not None:
        right = right - beta * (prev_ref[:PACKED] / left_ref[0, SQUARES : SQUARES + 1])
    right_ref[:PACKED] = right
    right_ref[PACKED:] = jnp.broadcast_to(beta, (IMAGE - PACKED, LANES))
    return jnp.sum(right * right, axis=0, keepdims=True)


def forward(first, green_ref, t0, t1, t2, t3, image_ref, *refs):
    prev_ref, left_ref, data_ref, right_ref = ((None, None) + refs) if first else refs
    ss = new_right(image_ref, right_ref, prev_ref, left_ref)
    model_to_data(right_ref, ss, green_ref, tables_of((t0, t1, t2, t3)), data_ref)


def last_right(image_ref, prev_ref, left_ref, right_ref, ss_ref):
    ss = new_right(image_ref, right_ref, prev_ref, left_ref)
    ss_ref[...] = jnp.broadcast_to(ss, (8, LANES))


def own_block(value, ref, rows_ref):
    rows_ref[...] = pltpu.roll(value, LANES - lax.axis_index(ZL) * 32, 1)
    for a in range(2):
        row = rows_ref[pl.ds(lax.axis_index(WIN) * 2 + a, 1), :]
        for one in range(2):
            ref[2 * a + one : 2 * a + one + 1, :] = row[:, one * 64 : one * 64 + 32]


def settle(v0_ref, v1_ref, v2_ref, u1_ref, u2_ref, image_ref, slip_ref, misfit_ref, right_ref, search_ref, rows_ref):
    zl = lax.axis_index(ZL)
    at = slice(PACKED, PACKED + 1)
    alphas = [ref[0, SQUARES : SQUARES + 1] for ref in (u1_ref, u2_ref)]
    betas = [ref[at] for ref in (v0_ref, v1_ref, v2_ref)]
    rights = [ref[:PACKED] / a for ref, a in zip((v0_ref, v1_ref), alphas)]
    phi_bar, rho_bar = betas[0], alphas[0]
    search, estimate = rights[0], jnp.zeros((PACKED, LANES), f32)
    for sweep in range(2):
        beta = betas[sweep + 1]
        rho = jnp.sqrt(rho_bar * rho_bar + beta * beta)
        cosine, sine = rho_bar / rho, beta / rho
        phi = cosine * phi_bar
        phi_bar = sine * phi_bar
        estimate = estimate + phi / rho * search
        if sweep == 0:
            rho_bar = -cosine * alphas[1]
            search = rights[1] - sine * alphas[1] / rho * search
        else:
            search = sine / rho * search
    own_block(estimate, slip_ref, rows_ref)
    own_block(v2_ref[:PACKED], right_ref, rows_ref)
    own_block(search, search_ref, rows_ref)
    own = u2_ref[lax.axis_index(STA)]
    source = lax.axis_index((Y, ZH, ZL)) ^ 1
    other = image_ref[source, HALF : HALF + PARTS, :].astype(f32) + image_ref[source, HALF + 8 : HALF + 8 + PARTS, :].astype(f32)
    for comp in range(COMP):
        rows = slice(2 * comp, 2 * comp + 2)
        for h in range(2):
            value = jnp.where(zl == h, own[rows], other[rows])
            misfit_ref[0, comp, :, h * LANES : (h + 1) * LANES] = value / betas[2] * phi_bar


def finish(s0, s1, s2, s3, right_ref, search_ref, direction_ref, scale):
    alpha = norm_of((s0[0:1] + s1[0:1]) + (s2[0:1] + s3[0:1]))[:, :32]
    direction_ref[...] = (right_ref[...] / alpha - alpha * search_ref[...]) * scale


def from_partners(array, axis, at=range(4)):
    held = {k: lax.ppermute(array, axis, [(at[i], at[i ^ k]) for i in range(4)]) for k in ORDER}
    return [held[k] for k in (1, 2, 3)]


def other_core(array):
    return lax.ppermute(array, C, [(0, 1), (1, 0)])


def add_cores(own_ref, other_ref, both_ref, sent_ref):
    both = own_ref[...] + other_ref[...]
    both_ref[...] = both
    sent_ref[...] = both.astype(bf16)
    squares = both[0, SQUARES : SQUARES + 1]
    sent_ref[0, SQUARES + 1 :, :] = (squares - squares.astype(bf16).astype(f32)).astype(bf16)


def along_x(array):
    side = lax.ppermute(array, (X, C), [(x * 2 + c, (x ^ (1, 3)[c]) * 2 + c) for x in range(4) for c in range(2)])
    across = lax.ppermute(array, X, [(x, x ^ 2) for x in range(4)])
    return [across, side, other_core(side)]


def data_over_patches(array):
    both, sent = call(add_cores, [(array.shape, f32), (array.shape, bf16)], array, other_core(array))
    return [both, *along_x(sent)]


def squares_over_patches(array):
    both = array + other_core(array)
    return [both, *along_x(both)]


def summed_over_frequencies(buf):
    return lax.all_to_all(buf, (Y, ZH, ZL), 0, 0, tiled=True)


def local(green, records, onsets, mask):
    packed = pack(mask, green, records).reshape(16, ROWS, LANES)
    packed, onset_rows = lax.optimization_barrier((packed, onsets.T[None]))
    arrived = lax.all_to_all(packed, STA, 0, 0, tiled=True)
    rows = jnp.concatenate([onset_rows, *from_partners(onset_rows, Y)], axis=0)
    gathered = jnp.stack([rows, *from_partners(rows, (ZL, ZH), (0, 2, 1, 3))])
    head, tail = ((SPLIT, LANES, LANES), f32), ((PACKED - SPLIT, LANES, LANES), f32)
    tables = call(table_body, [head, head], gathered)

    sent_shape, buf_shape = (((16, rows, LANES), bf16) for rows in (IMAGE, LAST_IMAGE))
    held = [pltpu.VMEM((LAST_IMAGE, LANES), f32)]
    data_shape, right_shape = ((16, 8, LANES), f32), ((IMAGE, LANES), f32)

    def forward_call(first, *args):
        return pl.pallas_call(
            functools.partial(forward, first),
            in_specs=[VMEM] * len(args),
            out_specs=[VMEM] * 2,
            out_shape=[jax.ShapeDtypeStruct(*data_shape), jax.ShapeDtypeStruct(*right_shape)],
            compiler_params=PARAMS,
            cost_estimate=pl.CostEstimate(flops=2_000_000, bytes_accessed=4_000_000, transcendentals=0),
        )(*args)

    buf, u0, *rest = call(first_adjoint, [sent_shape, data_shape, tail, tail], arrived, *tables, gathered, scratch=held)
    base = (arrived, *tables, *rest)
    data, v0 = forward_call(True, *base, summed_over_frequencies(buf))
    buf, u1 = call(next_adjoint, [sent_shape, data_shape], *base, *data_over_patches(data), u0, v0, scratch=held)
    data, v1 = forward_call(False, *base, summed_over_frequencies(buf), v0, u1)
    buf, u2 = call(next_adjoint, [buf_shape, data_shape], *base, *data_over_patches(data), u1, v1, scratch=held)
    image = summed_over_frequencies(buf)
    v2, ss = call(last_right, [right_shape, ((8, LANES), f32)], image, v1, u2)
    scale = math.sqrt(512 * 32)
    block = ((4, 32), f32)
    slip, misfit, right, search = call(
        settle, [block, ((1, COMP, 2, 256), f32), block, block], v0, v1, v2, u1, u2, image, scratch=[pltpu.VMEM((PACKED, LANES), f32)]
    )
    (direction,) = call(functools.partial(finish, scale=scale), [block], *squares_over_patches(ss), right, search)
    return slip.T, direction.T, misfit


def solution(mesh):
    finer = Mesh(mesh.devices.reshape(4, 2, 2, 4, 2), (X, ZL, C, Y, ZH))
    return jax.shard_map(
        local,
        mesh=finer,
        in_specs=(P(STA, None, None, None, WIN), P(STA, None, None, WIN), P(STA, WIN), P(STA, None)),
        out_specs=(P(STA, WIN), P(STA, WIN), P(STA, None, None, WIN)),
        check_vma=False,
    )
```
